8 devices in a mesh: data: 1 (over z), pp: 2 (over y), ep: 4 (over x, core).
Axes of the slice: x: 2, y: 2, z: 1, core: 2. Of those that a mesh axis runs over, the one named last changes fastest.
Arguments:
- expert_out: bfloat16 [2, 1, 128, 256, 4096], P(('data', 'pp'), None, 'ep')
- expert_ids: int32 [2, 1, 4, 512, 8], P(('data', 'pp'), None, 'ep')
- slot_ids: int32 [2, 1, 4, 512, 8], P(('data', 'pp'), None, 'ep')
- gates: float32 [2, 1, 4, 512, 8], P(('data', 'pp'), None, 'ep')
- resid: bfloat16 [2, 1, 4, 512, 4096], P(('data', 'pp'), None, 'ep')
- norm_scale: float32 [2, 4096], P('pp')
- w_query: bfloat16 [2, 4096, 12288], P('pp')
- w_key: bfloat16 [2, 4096, 12288], P('pp')
- w_value: bfloat16 [2, 4096, 12288], P('pp')
- w_out: bfloat16 [2, 96, 128, 4096], P('pp')
Outputs:
- output: bfloat16 [2, 1, 4, 512, 4096], P(('data', 'pp'), None, 'ep')
All inputs are finite; a program needn't handle non-finite values.
Results may differ from the reference program's by a relative error of at most 0.0123938.
Values are sent between devices in bfloat16 or wider.
A program may use at most 2 GiB of HBM per device.

```python
import jax
import jax.numpy as jnp
from jax import lax

STAGES = 2
EP_DEVS = 4
MICRO = 1
SEQ_DEV = 1
SEQ_LEN = 512
MODEL_DIM = 4096
EXPERTS = 128
TOP_K = 8
HEADS = 96
HEAD_DIM = 128

TOK_DEV = SEQ_DEV * SEQ_LEN
TOKENS = TOK_DEV * EP_DEVS
SEQ_COUNT = SEQ_DEV * EP_DEVS
SLOT_DEV = 2 * TOK_DEV * TOP_K // EXPERTS
CAPACITY = SLOT_DEV * EP_DEVS
HOT_EXPERTS = EXPERTS // 4
HOT_PICKS = TOP_K // 2
HIDDEN = HEADS * HEAD_DIM
NORM_EPS = 1e-6
TOKEN_SHAPE = (STAGES, MICRO, SEQ_COUNT, SEQ_LEN)


def rank_in_group(group_ids):
    count = group_ids.shape[0]
    order = jnp.argsort(group_ids * count + jnp.arange(count))
    sorted_ids = group_ids[order]
    first_pos = jnp.searchsorted(sorted_ids, sorted_ids, side='left')
    sorted_rank = (jnp.arange(count) - first_pos).astype(jnp.int32)
    return jnp.zeros((count,), jnp.int32).at[order].set(sorted_rank)


def draw_group(group_key):
    perm_key, hot_key, cold_key = jax.random.split(group_key, 3)
    expert_order = jax.random.permutation(perm_key, EXPERTS)
    hot_list = expert_order[:HOT_EXPERTS]
    cold_list = expert_order[HOT_EXPERTS:]
    hot_score = jax.random.randint(hot_key, (TOKENS, HOT_EXPERTS), 0, 65536) * HOT_EXPERTS + jnp.arange(HOT_EXPERTS)
    cold_score = jax.random.randint(cold_key, (TOKENS, EXPERTS - HOT_EXPERTS), 0, 65536) * EXPERTS + jnp.arange(EXPERTS - HOT_EXPERTS)
    hot_pick = jnp.argsort(hot_score, axis=1)[:, :HOT_PICKS]
    cold_pick = jnp.argsort(cold_score, axis=1)[:, :TOP_K - HOT_PICKS]
    chosen = jnp.concatenate([hot_list[hot_pick], cold_list[cold_pick]], axis=1).astype(jnp.int32)
    ranks = jax.vmap(rank_in_group)(chosen.reshape(EP_DEVS, TOK_DEV * TOP_K))
    slot_base = (jnp.arange(EP_DEVS, dtype=jnp.int32) * SLOT_DEV)[:, None]
    slots = jnp.where(ranks < SLOT_DEV, ranks + slot_base, -1).astype(jnp.int32)
    return chosen, slots.reshape(TOKENS, TOP_K)


def draw_routing(route_key):
    group_keys = jax.random.split(route_key, STAGES * MICRO)
    chosen, slots = lax.map(draw_group, group_keys)
    full_shape = TOKEN_SHAPE + (TOP_K,)
    return chosen.reshape(full_shape), slots.reshape(full_shape)


def draw_stage_out(stage_key):
    scale_key, value_key = jax.random.split(stage_key)
    expert_scale = jnp.exp(0.5 * jax.random.normal(scale_key, (MICRO, EXPERTS, 1, 1), jnp.float32))
    raw_out = jax.random.normal(value_key, (MICRO, EXPERTS, CAPACITY, MODEL_DIM), jnp.float32)
    return (raw_out * expert_scale).astype(jnp.bfloat16)


def setup_inputs(seed: int = 0, part: int = 0) -> dict:
    part_key = jax.random.fold_in(jax.random.key(seed), part)
    route_key, gate_key, resid_key, out_key = jax.random.split(part_key, 4)
    shared = jax.random.split(jax.random.key(seed + 1), 5)
    expert_ids, slot_ids = draw_routing(route_key)
    gate_logits = 1.5 * jax.random.normal(gate_key, TOKEN_SHAPE + (TOP_K,), jnp.float32)
    gates = 2.0 * jax.nn.softmax(gate_logits, axis=-1)
    resid = jax.random.normal(resid_key, TOKEN_SHAPE + (MODEL_DIM,), jnp.float32).astype(jnp.bfloat16)
    expert_out = lax.map(draw_stage_out, jax.random.split(out_key, STAGES))
    norm_scale = 1.0 + 0.5 * jax.random.normal(shared[0], (STAGES, MODEL_DIM), jnp.float32)
    in_scale = MODEL_DIM ** -0.5
    w_query = (1.5 * in_scale * jax.random.normal(shared[1], (STAGES, MODEL_DIM, HIDDEN), jnp.float32)).astype(jnp.bfloat16)
    w_key = (in_scale * jax.random.normal(shared[2], (STAGES, MODEL_DIM, HIDDEN), jnp.float32)).astype(jnp.bfloat16)
    w_value = (in_scale * jax.random.normal(shared[3], (STAGES, MODEL_DIM, HIDDEN), jnp.float32)).astype(jnp.bfloat16)
    w_out = (2.0 * HIDDEN ** -0.5 * jax.random.normal(shared[4], (STAGES, HEADS, HEAD_DIM, MODEL_DIM), jnp.float32)).astype(jnp.bfloat16)
    return {'expert_out': expert_out, 'expert_ids': expert_ids, 'slot_ids': slot_ids, 'gates': gates, 'resid': resid, 'norm_scale': norm_scale, 'w_query': w_query, 'w_key': w_key, 'w_value': w_value, 'w_out': w_out}


def combine_group(group_args):
    row_table, flat_ids, weights, resid_rows = group_args
    running = resid_rows.astype(jnp.float32)
    for choice in range(TOP_K):
        running = running + weights[:, choice, None] * row_table[flat_ids[:, choice]].astype(jnp.float32)
    return running.astype(jnp.bfloat16)


def attend_sequence(seq_rows, gain_row, w_query, w_key, w_value, w_out):
    x_float = seq_rows.astype(jnp.float32)
    inv_rms = lax.rsqrt(jnp.mean(x_float * x_float, axis=-1, keepdims=True) + NORM_EPS)
    normed = (x_float * inv_rms * gain_row).astype(jnp.bfloat16)
    q_heads = jnp.dot(normed, w_query, preferred_element_type=jnp.float32).astype(jnp.bfloat16).reshape(SEQ_LEN, HEADS, HEAD_DIM)
    k_heads = jnp.dot(normed, w_key, preferred_element_type=jnp.float32).astype(jnp.bfloat16).reshape(SEQ_LEN, HEADS, HEAD_DIM)
    v_heads = jnp.dot(normed, w_value, preferred_element_type=jnp.float32).astype(jnp.bfloat16).reshape(SEQ_LEN, HEADS, HEAD_DIM)
    scores = jnp.einsum('qhe,khe->hqk', q_heads.astype(jnp.float32), k_heads.astype(jnp.float32)) * HEAD_DIM ** -0.5
    positions = jnp.arange(SEQ_LEN)
    causal = positions[:, None] >= positions[None, :]
    attn_prob = jax.nn.softmax(jnp.where(causal, scores, -jnp.inf), axis=-1).astype(jnp.bfloat16)
    context = jnp.einsum('hqk,khe->qhe', attn_prob.astype(jnp.float32), v_heads.astype(jnp.float32)).astype(jnp.bfloat16)
    proj = jnp.einsum('qhe,hed->qd', context.astype(jnp.float32), w_out.astype(jnp.float32)).astype(jnp.bfloat16)
    return (x_float + proj.astype(jnp.float32)).astype(jnp.bfloat16)


def reference(expert_out, expert_ids, slot_ids, gates, resid, norm_scale, w_query, w_key, w_value, w_out):
    groups = STAGES * MICRO
    row_table = expert_out.reshape(groups, EXPERTS * CAPACITY, MODEL_DIM)
    is_kept = slot_ids >= 0
    flat_ids = (expert_ids * CAPACITY + jnp.where(is_kept, slot_ids, 0)).reshape(groups, TOKENS, TOP_K)
    weights = jnp.where(is_kept, gates, 0.0).reshape(groups, TOKENS, TOP_K)
    resid_rows = resid.reshape(groups, TOKENS, MODEL_DIM)
    combined = lax.map(combine_group, (row_table, flat_ids, weights, resid_rows))
    shifted = jnp.roll(combined.reshape(STAGES, MICRO * SEQ_COUNT, SEQ_LEN, MODEL_DIM), 1, axis=0)

    def stage_block(stage_args):
        stage_seqs, gain_row, stage_query, stage_key, stage_value, stage_out = stage_args

        def one_sequence(seq_rows):
            return attend_sequence(seq_rows, gain_row, stage_query, stage_key, stage_value, stage_out)

        return lax.map(one_sequence, stage_seqs)

    result = lax.map(stage_block, (shifted, norm_scale, w_query, w_key, w_value, w_out))
    return result.reshape(TOKEN_SHAPE + (MODEL_DIM,))
```

```python
import functools

import jax
import jax.numpy as jnp
from jax import lax
from jax.experimental import pallas as pl
from jax.experimental.pallas import tpu as pltpu
from jax.sharding import PartitionSpec as P

NORM_EPS = 1e-6
LANES = 128
VMEM_LIMIT = 60 * 2**20
PART_COLS = 512
ADD_COLS = 1024
PROJ_COLS = 512
FIRST_CHUNKS = (64, 128, 64)
LAST_CHUNKS = (64, 128, 64)
ANY_SPEC = pl.BlockSpec(memory_space=pl.ANY)
VMEM_SPEC = pl.BlockSpec(memory_space=pltpu.VMEM)


def fill_gate_terms(table, first_code, terms_ref):
    rows = table.shape[0]
    top_k = table.shape[1] // 2
    slots = terms_ref.shape[1]
    lane_ids = lax.broadcasted_iota(jnp.int32, (rows, LANES), 1).astype(jnp.float32)
    codes = [jnp.broadcast_to(table[:, j:j + 1] - first_code, (rows, LANES)) for j in range(top_k)]
    gates = [jnp.broadcast_to(table[:, top_k + j:top_k + j + 1], (rows, LANES)) for j in range(top_k)]
    for tile in range(slots // LANES):
        here = lane_ids + float(tile * LANES)
        gate = jnp.zeros((rows, LANES), jnp.float32)
        for j in range(top_k):
            gate = jnp.where(codes[j] == here, gates[j], gate)
        high = gate.astype(jnp.bfloat16)
        rest = gate - high.astype(jnp.float32)
        middle = rest.astype(jnp.bfloat16)
        low = (rest - middle.astype(jnp.float32)).astype(jnp.bfloat16)
        cols = pl.ds(tile * LANES, LANES)
        terms_ref[pl.ds(0, rows), cols] = high
        terms_ref[pl.ds(rows, rows), cols] = middle
        terms_ref[pl.ds(2 * rows, rows), cols] = low


def normalise(x_ref, gain_ref, normed_ref):
    for first in range(0, x_ref.shape[0], 64):
        x_float = x_ref[first:first + 64].astype(jnp.float32)
        inv_rms = lax.rsqrt(jnp.mean(jnp.square(x_float), axis=-1, keepdims=True) + NORM_EPS)
        normed_ref[first:first + 64] = (x_float * inv_rms * gain_ref[...]).astype(jnp.bfloat16)


def exchange_kernel(table_ref, out_rows_ref, resid_ref, gain_ref, wq_ref, wk_ref, wv_ref,
                    arrived_ref, q_ref, k_ref, v_ref,
                    pair_out_ref, pair_in_ref, cross_out_ref, cross_in_ref,
                    near_out_ref, near_in_ref, base_ref, combined_ref,
                    terms_ref, x_ref, normed_ref, load_sem, send_sems, recv_sems):
    me = lax.axis_index('ep')
    stage = lax.axis_index('pp')
    model_dim = resid_ref.shape[1]
    experts = out_rows_ref.shape[0]
    slot_dev = out_rows_ref.shape[1] // table_ref.shape[0]
    first_code = (me * (experts * slot_dev)).astype(jnp.float32)
    partner, across, diagonal = me ^ 1, me ^ 2, me ^ 3
    next_stage = 1 - stage

    barrier = pltpu.get_barrier_semaphore()
    pl.semaphore_signal(barrier, inc=1, device_id={'ep': partner}, device_id_type=pl.DeviceIdType.MESH)
    pl.semaphore_signal(barrier, inc=1, device_id={'ep': across}, device_id_type=pl.DeviceIdType.MESH)
    pl.semaphore_signal(barrier, inc=1, device_id={'pp': next_stage}, device_id_type=pl.DeviceIdType.MESH)
    pl.semaphore_wait(barrier, 3)

    copies = []

    def send(src_ref, dst_ref, start, rows, target):
        index = len(copies)
        span = pl.ds(start, rows)
        copy = pltpu.make_async_remote_copy(
            src_ref=src_ref.at[span], dst_ref=dst_ref.at[span],
            send_sem=send_sems.at[index], recv_sem=recv_sems.at[index],
            device_id=target, device_id_type=pl.DeviceIdType.MESH)
        copy.start()
        copies.append(copy)
        return copy

    def partial_sums(owner, start, rows, addends, dst_ref):
        fill_gate_terms(table_ref[owner, start:start + rows], first_code, terms_ref.at[pl.ds(0, 3 * rows)])

        def body(block_ref, *refs):
            total_ref = refs[-1]
            block = block_ref[...].reshape(experts * slot_dev, PART_COLS)
            sums = jnp.dot(terms_ref[0:3 * rows], block, preferred_element_type=jnp.float32)
            total = sums[:rows] + (sums[rows:2 * rows] + sums[2 * rows:])
            for ref in refs[:-1]:
                total = ref[...].astype(jnp.float32) + total
            total_ref[...] = total

        row_spec = pl.BlockSpec((rows, PART_COLS), lambda n: (0, n))
        pltpu.emit_pipeline(
            body, grid=(model_dim // PART_COLS,),
            in_specs=[pl.BlockSpec((experts, slot_dev, PART_COLS), lambda n: (0, owner, n))] + [row_spec] * len(addends),
            out_specs=[row_spec],
        )(out_rows_ref, *[ref.at[pl.ds(start, rows)] for ref in addends], dst_ref.at[pl.ds(start, rows)])

    def finish(start, rows):
        def body(base_block, cross_block, out_block):
            out_block[...] = (base_block[...] + cross_block[...]).astype(jnp.bfloat16)

        span = pl.ds(start, rows)
        spec = pl.BlockSpec((rows, ADD_COLS), lambda n: (0, n))
        pltpu.emit_pipeline(body, grid=(model_dim // ADD_COLS,), in_specs=[spec, spec], out_specs=[spec])(
            base_ref.at[span], cross_in_ref.at[span], combined_ref.at[span])
        return send(combined_ref, arrived_ref, start, rows, {'pp': next_stage})

    def project(w_ref, dst_ref, first, count):
        def body(w_block, out_block):
            out_block[...] = jnp.dot(normed_ref[...], w_block[...], preferred_element_type=jnp.float32).astype(jnp.bfloat16)

        pltpu.emit_pipeline(
            body, grid=(count,),
            in_specs=[pl.BlockSpec((model_dim, PROJ_COLS), lambda n: (0, n + first))],
            out_specs=[pl.BlockSpec((normed_ref.shape[0], PROJ_COLS), lambda n: (0, n + first))],
        )(w_ref, dst_ref)

    spans, start = [], 0
    for rows in FIRST_CHUNKS + LAST_CHUNKS:
        spans.append((start, rows))
        start += rows
    n_first = len(FIRST_CHUNKS)
    half = sum(FIRST_CHUNKS)

    def pair_part(c):
        partial_sums(diagonal, *spans[c], (), pair_out_ref)
        return send(pair_out_ref, pair_in_ref, *spans[c], {'ep': partner})

    def cross_part(c, pair):
        pair.wait_recv()
        partial_sums(across, *spans[c], (pair_in_ref,), cross_out_ref)
        return send(cross_out_ref, cross_in_ref, *spans[c], {'ep': across})

    def near_part(part):
        partial_sums(partner, part * half, half, (), near_out_ref)
        return send(near_out_ref, near_in_ref, part * half, half, {'ep': partner})

    def base_part(part, near):
        near.wait_recv()
        partial_sums(me, part * half, half, (resid_ref, near_in_ref), base_ref)

    pairs, cross, moved = {}, {}, {}

    def finish_chunk(c):
        cross[c].wait_recv()
        moved[c] = finish(*spans[c])

    pairs[0] = pair_part(0)
    pairs[1] = pair_part(1)
    cross[0] = cross_part(0, pairs[0])
    cross[1] = cross_part(1, pairs[1])
    pairs[2] = pair_part(2)
    near_0 = near_part(0)
    cross[2] = cross_part(2, pairs[2])
    pairs[3] = pair_part(3)
    base_part(0, near_0)
    finish_chunk(0)
    cross[3] = cross_part(3, pairs[3])
    pairs[4] = pair_part(4)
    pairs[5] = pair_part(5)
    cross[4] = cross_part(4, pairs[4])
    finish_chunk(1)
    cross[5] = cross_part(5, pairs[5])
    near_1 = near_part(1)
    finish_chunk(2)
    base_part(1, near_1)

    for c in range(n_first):
        moved[c].wait_recv()
    load = pltpu.make_async_copy(arrived_ref.at[pl.ds(0, half)], x_ref, load_sem)
    load.start()
    load.wait()
    normalise(x_ref, gain_ref, normed_ref)
    steps = q_ref.shape[1] // PROJ_COLS
    project(wq_ref, q_ref, 0, steps)
    finish_chunk(3)
    project(wk_ref, k_ref, 0, steps)
    project(wv_ref, v_ref, 0, steps // 3)
    finish_chunk(4)
    project(wv_ref, v_ref, steps // 3, steps // 3)
    finish_chunk(5)
    project(wv_ref, v_ref, 2 * (steps // 3), steps - 2 * (steps // 3))
    for c in range(n_first, len(spans)):
        moved[c].wait_recv()
    for copy in copies:
        copy.wait_send()


def exchange(table, own_out, own_resid, gain, w_query, w_key, w_value):
    seq, model_dim = own_resid.shape
    hidden = w_query.shape[1]
    half = sum(FIRST_CHUNKS)
    slots = own_out.shape[0] * own_out.shape[1] // table.shape[0]
    wide = jax.ShapeDtypeStruct((seq, model_dim), jnp.float32)
    narrow = jax.ShapeDtypeStruct((seq, model_dim), jnp.bfloat16)
    heads_out = jax.ShapeDtypeStruct((half, hidden), jnp.bfloat16)
    out_shape = [narrow, heads_out, heads_out, heads_out] + [wide] * 7 + [narrow]
    n_copies = 3 * len(FIRST_CHUNKS + LAST_CHUNKS) + 2
    outs = pl.pallas_call(
        exchange_kernel,
        out_shape=out_shape,
        in_specs=[VMEM_SPEC, ANY_SPEC, ANY_SPEC, VMEM_SPEC, ANY_SPEC, ANY_SPEC, ANY_SPEC],
        out_specs=[ANY_SPEC] * len(out_shape),
        scratch_shapes=[
            pltpu.VMEM((3 * half, slots), jnp.bfloat16),
            pltpu.VMEM((half, model_dim), jnp.bfloat16),
            pltpu.VMEM((half, model_dim), jnp.bfloat16),
            pltpu.SemaphoreType.DMA,
            pltpu.SemaphoreType.DMA((n_copies,)),
            pltpu.SemaphoreType.DMA((n_copies,)),
        ],
        compiler_params=pltpu.CompilerParams(vmem_limit_bytes=VMEM_LIMIT, collective_id=0, has_side_effects=True),
        name="exchange",
    )(table, own_out, own_resid, gain, w_query, w_key, w_value)
    return outs[:4]


def project_kernel(gain_ref, x_ref, w_ref, out_ref, normed_ref):
    @pl.when(pl.program_id(0) == 0)
    def _():
        normalise(x_ref, gain_ref, normed_ref)

    out_ref[...] = jnp.dot(normed_ref[...], w_ref[...], preferred_element_type=jnp.float32).astype(jnp.bfloat16)


def project(arrived, part, rows, gain, w_mat):
    model_dim, hidden = w_mat.shape
    return pl.pallas_call(
        project_kernel,
        out_shape=jax.ShapeDtypeStruct((rows, hidden), jnp.bfloat16),
        grid=(hidden // PROJ_COLS,),
        in_specs=[
            pl.BlockSpec(gain.shape, lambda n: (0, 0)),
            pl.BlockSpec((rows, model_dim), lambda n: (part, 0)),
            pl.BlockSpec((model_dim, PROJ_COLS), lambda n: (0, n)),
        ],
        out_specs=pl.BlockSpec((rows, PROJ_COLS), lambda n: (0, n)),
        scratch_shapes=[pltpu.VMEM((rows, model_dim), jnp.bfloat16)],
        compiler_params=pltpu.CompilerParams(vmem_limit_bytes=VMEM_LIMIT, dimension_semantics=("arbitrary",)),
        cost_estimate=pl.CostEstimate(flops=2 * rows * model_dim * hidden, bytes_accessed=2 * model_dim * hidden + 2 * rows * hidden, transcendentals=0),
        name="project",
    )(gain, arrived, w_mat)


def attend_kernel(head_dim, parts, *refs):
    q_ref, k_refs, v_refs, out_ref = refs[0], refs[1:1 + parts], refs[1 + parts:1 + 2 * parts], refs[-1]
    rows = q_ref.shape[0]
    heads = q_ref.shape[1] // head_dim
    scale = head_dim ** -0.5
    q_pos = lax.broadcasted_iota(jnp.int32, (rows, rows), 0)
    k_pos = lax.broadcasted_iota(jnp.int32, (rows, rows), 1)
    causal = q_pos >= k_pos
    for h in range(heads):
        cols = pl.ds(h * head_dim, head_dim)
        query = q_ref[:, cols]
        scores = [
            lax.dot_general(query, ref[:, cols], (((1,), (1,)), ((), ())), preferred_element_type=jnp.float32) * scale
            for ref in k_refs
        ]
        scores[-1] = jnp.where(causal, scores[-1], -jnp.inf)
        top = scores[0].max(axis=-1, keepdims=True)
        for s in scores[1:]:
            top = jnp.maximum(top, s.max(axis=-1, keepdims=True))
        weights = [jnp.exp(s - top) for s in scores]
        total = weights[0].sum(axis=-1, keepdims=True)
        for w in weights[1:]:
            total = total + w.sum(axis=-1, keepdims=True)
        inverse = 1.0 / total
        mixed = jnp.zeros((rows, head_dim), jnp.float32)
        for w, ref in zip(weights, v_refs):
            mixed = mixed + jnp.dot((w * inverse).astype(jnp.bfloat16), ref[:, cols], preferred_element_type=jnp.float32)
        out_ref[:, cols] = mixed.astype(jnp.bfloat16)


def attend(query, keys, values, head_dim, total_parts, context=None):
    rows, hidden = query.shape
    parts = len(keys)
    step = 4 * head_dim
    spec = pl.BlockSpec((rows, step), lambda h: (0, h))
    held = [] if context is None else [context]
    return pl.pallas_call(
        functools.partial(attend_kernel, head_dim, parts),
        out_shape=jax.ShapeDtypeStruct((rows * total_parts, hidden), jnp.bfloat16),
        grid=(hidden // step,),
        in_specs=[spec] * (1 + 2 * parts) + [ANY_SPEC] * len(held),
        out_specs=pl.BlockSpec((rows, step), lambda h: (parts - 1, h)),
        input_output_aliases={1 + 2 * parts: 0} if held else {},
        compiler_params=pltpu.CompilerParams(vmem_limit_bytes=VMEM_LIMIT, dimension_semantics=("arbitrary",)),
        cost_estimate=pl.CostEstimate(flops=4 * rows * rows * parts * hidden, bytes_accessed=4 * rows * (1 + parts) * hidden, transcendentals=rows * rows * parts * hidden // head_dim),
        name="attend",
    )(query, *keys, *values, *held)


def solution(mesh):
    ep_size = mesh.shape['ep']
    token_spec = P(('data', 'pp'), None, 'ep', None, None)
    weight_spec = P('pp', None, None)

    def local_step(expert_out, expert_ids, slot_ids, gates, resid, norm_scale, w_query, w_key, w_value, w_out):
        own_out = expert_out[0, 0]
        own_resid = resid[0, 0, 0]
        model_dim = own_out.shape[2]
        slot_dev = own_out.shape[1] // ep_size
        me = lax.axis_index('ep')
        ids, slots, own_gates = expert_ids[0, 0, 0], slot_ids[0, 0, 0], gates[0, 0, 0]
        code = jnp.where(slots >= 0, ids * slot_dev + (slots - me * slot_dev), -1).astype(jnp.float32)
        own_table = jnp.concatenate([code.T, own_gates.T], axis=0)
        table = lax.all_gather(own_table, 'ep').transpose(0, 2, 1)
        gain = norm_scale.reshape(1, model_dim)
        arrived, query_1, key_1, value_1 = exchange(table, own_out, own_resid, gain, w_query[0], w_key[0], w_value[0])

        head_count, head_dim = w_out.shape[1], w_out.shape[2]
        half = query_1.shape[0]
        context = attend(query_1, [key_1], [value_1], head_dim, 2)
        query_2, key_2, value_2 = [project(arrived, 1, half, gain, w[0]) for w in (w_query, w_key, w_value)]
        context = attend(query_2, [key_1, key_2], [value_1, value_2], head_dim, 2, context)
        flat_out = w_out[0].reshape(head_count * head_dim, model_dim)
        proj = jnp.dot(context, flat_out, preferred_element_type=jnp.float32).astype(jnp.bfloat16)
        result = (arrived.astype(jnp.float32) + proj.astype(jnp.float32)).astype(jnp.bfloat16)
        return result[None, None, None]

    return jax.shard_map(local_step, mesh=mesh, in_specs=(token_spec, token_spec, token_spec, token_spec, token_spec, P('pp', None), weight_spec, weight_spec, weight_spec, P('pp', None, None, None)), out_specs=token_spec, check_vma=False)
```

```python
import functools

import jax
import jax.numpy as jnp
from jax import lax
from jax.experimental import pallas as pl
from jax.experimental.pallas import tpu as pltpu
from jax.sharding import PartitionSpec as P

NORM_EPS = 1e-6
LANES = 128
VMEM_LIMIT = 62 * 2**20
PART_COLS = 512
SEND_COLS = 1024
HEAD_GROUP = 2
WEIGHT_BUFFERS = 3
HALVES = 2
ANY_SPEC = pl.BlockSpec(memory_space=pl.ANY)
VMEM_SPEC = pl.BlockSpec(memory_space=pltpu.VMEM)


def fill_gate_terms(table_ref, first_row, first_code, terms_ref):
    rows = terms_ref.shape[0] // 3
    slots = terms_ref.shape[1]
    top_k = table_ref.shape[1] // 2
    step = 32

    @pl.loop(0, rows // step)
    def _(i):
        table = table_ref[pl.ds(pl.multiple_of(first_row + i * step, step), step), :]
        lane_ids = lax.broadcasted_iota(jnp.int32, (step, LANES), 1).astype(jnp.float32)
        codes = [jnp.broadcast_to(table[:, j:j + 1] - first_code, (step, LANES)) for j in range(top_k)]
        gates = [jnp.broadcast_to(table[:, top_k + j:top_k + j + 1], (step, LANES)) for j in range(top_k)]
        for tile in range(slots // LANES):
            here = lane_ids + float(tile * LANES)
            gate = jnp.zeros((step, LANES), jnp.float32)
            for j in range(top_k):
                gate = jnp.where(codes[j] == here, gates[j], gate)
            high = gate.astype(jnp.bfloat16)
            rest = gate - high.astype(jnp.float32)
            middle = rest.astype(jnp.bfloat16)
            low = (rest - middle.astype(jnp.float32)).astype(jnp.bfloat16)
            for k, term in enumerate((high, middle, low)):
                at = pl.ds(pl.multiple_of(k * rows + i * step, step), step)
                terms_ref[at, tile * LANES:(tile + 1) * LANES] = term


def normalise(x_ref, gain_ref, normed_ref):
    for first in range(0, x_ref.shape[0], 64):
        x_float = x_ref[first:first + 64].astype(jnp.float32)
        inv_rms = lax.rsqrt(jnp.mean(jnp.square(x_float), axis=-1, keepdims=True) + NORM_EPS)
        normed_ref[first:first + 64] = (x_float * inv_rms * gain_ref[...]).astype(jnp.bfloat16)


def attend_heads(queries, key_parts, value_parts, head_dim, out_ref):
    rows = queries.shape[0]
    scale = head_dim ** -0.5
    q_pos = lax.broadcasted_iota(jnp.int32, (rows, rows), 0)
    k_pos = lax.broadcasted_iota(jnp.int32, (rows, rows), 1)
    causal = q_pos >= k_pos
    for first in range(0, queries.shape[1], head_dim):
        cols = slice(first, first + head_dim)
        query = queries[:, cols]
        scores = [
            lax.dot_general(query, keys[:, cols], (((1,), (1,)), ((), ())), preferred_element_type=jnp.float32) * scale
            for keys in key_parts
        ]
        scores[-1] = jnp.where(causal, scores[-1], -jnp.inf)
        top = scores[0].max(axis=-1, keepdims=True)
        for s in scores[1:]:
            top = jnp.maximum(top, s.max(axis=-1, keepdims=True))
        weights = [jnp.exp(s - top) for s in scores]
        total = weights[0].sum(axis=-1, keepdims=True)
        for w in weights[1:]:
            total = total + w.sum(axis=-1, keepdims=True)
        inverse = 1.0 / total
        mixed = jnp.zeros((rows, head_dim), jnp.float32)
        for w, values in zip(weights, value_parts):
            mixed = mixed + jnp.dot((w * inverse).astype(jnp.bfloat16), values[:, cols], preferred_element_type=jnp.float32)
        out_ref[:, cols] = mixed.astype(jnp.bfloat16)


def project_block(normed_ref, w_ref):
    return jnp.dot(normed_ref[...], w_ref[...], preferred_element_type=jnp.float32).astype(jnp.bfloat16)


def weight_spec_at(model_dim, cols, first):
    return pl.BlockSpec((model_dim, cols), lambda n: (0, n + first), pipeline_mode=pl.Buffered(WEIGHT_BUFFERS))


def exchange_kernel(head_dim, table_ref, out_rows_ref, resid_ref, gain_ref, wq_ref, wk_ref, wv_ref,
                    arrived_ref, k_ref, v_ref, context_ref, pair_out_ref, cross_out_ref, near_out_ref,
                    terms_ref, pair_in_ref, near_in_ref, cross_in_ref, base_ref, combined_ref, x_ref, normed_ref,
                    load_sem, send_sems, recv_sems):
    me = lax.axis_index('ep')
    stage = lax.axis_index('pp')
    seq, model_dim = resid_ref.shape
    half = seq // HALVES
    experts = out_rows_ref.shape[0]
    slot_dev = out_rows_ref.shape[1] // table_ref.shape[0]
    first_code = (me * (experts * slot_dev)).astype(jnp.float32)
    partner, across, diagonal = me ^ 1, me ^ 2, me ^ 3
    next_stage = 1 - stage

    barrier = pltpu.get_barrier_semaphore()
    pl.semaphore_signal(barrier, inc=1, device_id={'ep': partner}, device_id_type=pl.DeviceIdType.MESH)
    pl.semaphore_signal(barrier, inc=1, device_id={'ep': across}, device_id_type=pl.DeviceIdType.MESH)
    pl.semaphore_signal(barrier, inc=1, device_id={'pp': next_stage}, device_id_type=pl.DeviceIdType.MESH)
    pl.semaphore_wait(barrier, 3)

    copies = []

    def send(src_ref, dst_ref, target):
        index = len(copies)
        copy = pltpu.make_async_remote_copy(
            src_ref=src_ref, dst_ref=dst_ref, send_sem=send_sems.at[index], recv_sem=recv_sems.at[index],
            device_id=target, device_id_type=pl.DeviceIdType.MESH)
        copy.start()
        copies.append(copy)
        return copy

    def fill(slot, owner, part):
        fill_gate_terms(table_ref.at[owner], part * half, first_code, terms_ref.at[slot])

    def partial_sums(slot, owner, first, cols, dst_ref, extra_ref=None, resid=None, keep_ref=None):
        steps, begin = cols // PART_COLS, first // PART_COLS

        def body(block_ref, *refs):
            block = block_ref[...].reshape(experts * slot_dev, PART_COLS)
            sums = jnp.dot(terms_ref[slot], block, preferred_element_type=jnp.float32)
            total = sums[:half] + (sums[half:2 * half] + sums[2 * half:])
            at = pl.ds(pl.multiple_of((pl.program_id(0) + begin) * PART_COLS, PART_COLS), PART_COLS)
            if extra_ref is not None:
                total = total + extra_ref[:, at]
            if resid is not None:
                total = refs[0][...].astype(jnp.float32) + total
            if keep_ref is not None:
                keep_ref[:, at] = total
            else:
                refs[-1][...] = total

        col_spec = pl.BlockSpec((half, PART_COLS), lambda n: (0, n + begin))
        in_specs = [pl.BlockSpec((experts, slot_dev, PART_COLS), lambda n: (0, owner, n + begin))]
        operands = [out_rows_ref]
        if resid is not None:
            in_specs.append(col_spec)
            operands.append(resid)
        if keep_ref is None:
            pltpu.emit_pipeline(body, grid=(steps,), in_specs=in_specs, out_specs=[col_spec])(*operands, dst_ref)
        else:
            pltpu.emit_pipeline(body, grid=(steps,), in_specs=in_specs)(*operands)

    def col_span(first, cols):
        return (slice(None), pl.ds(first, cols))

    def half_rows(part):
        return pl.ds(part * half, half)

    def pair_part(part, first, cols):
        source = pair_out_ref.at[part]
        partial_sums(0, diagonal, first, cols, source)
        span = col_span(first, cols)
        return send(source.at[span], pair_in_ref.at[span], {'ep': partner})

    def cross_part(part, first, cols, pair):
        pair.wait_recv()
        source = cross_out_ref.at[part]
        partial_sums(1, across, first, cols, source, extra_ref=pair_in_ref)
        for at in range(first, first + cols, SEND_COLS):
            span = col_span(at, SEND_COLS)
            crossed[part].append(send(source.at[span], cross_in_ref.at[part].at[span], {'ep': across}))

    def near_part(part):
        source = near_out_ref.at[part]
        partial_sums(0, partner, 0, model_dim, source)
        return send(source, near_in_ref, {'ep': partner})

    def base_part(part, near):
        near.wait_recv()
        partial_sums(1, me, 0, model_dim, None, extra_ref=near_in_ref, resid=resid_ref.at[half_rows(part)], keep_ref=base_ref)

    def finish(part, index):
        if part > 0:
            moved[part - 1][index].wait_send()
        crossed[part][index].wait_recv()
        span = col_span(index * SEND_COLS, SEND_COLS)
        combined_ref[span] = (base_ref[span] + cross_in_ref[(part,) + span]).astype(jnp.bfloat16)
        target = arrived_ref.at[half_rows(part), pl.ds(index * SEND_COLS, SEND_COLS)]
        moved[part].append(send(combined_ref.at[span], target, {'pp': next_stage}))

    crossed = [[], []]
    moved = [[], []]
    chunks = model_dim // SEND_COLS
    one, rest = SEND_COLS, model_dim - 2 * SEND_COLS
    fill(0, diagonal, 0)
    pair_a = pair_part(0, 0, one)
    fill(1, across, 0)
    cross_part(0, 0, one, pair_a)
    pair_b = pair_part(0, one, one)
    pair_c = pair_part(0, 2 * one, rest)
    cross_part(0, one, one, pair_b)
    cross_part(0, 2 * one, rest, pair_c)
    fill(0, partner, 0)
    near = near_part(0)
    fill(1, me, 0)
    base_part(0, near)
    finish(0, 0)
    finish(0, 1)
    fill(0, diagonal, 1)
    pair_d = pair_part(1, 0, model_dim)
    finish(0, 2)
    fill(1, across, 1)
    cross_part(1, 0, model_dim, pair_d)
    for index in range(3, chunks):
        finish(0, index)
    fill(0, partner, 1)
    near = near_part(1)
    fill(1, me, 1)

    for copy in moved[0]:
        copy.wait_recv()
    load = pltpu.make_async_copy(arrived_ref.at[half_rows(0)], x_ref, load_sem)
    load.start()
    load.wait()
    normalise(x_ref, gain_ref, normed_ref)

    group = HEAD_GROUP * head_dim
    groups = k_ref.shape[1] // group

    def head_groups(first, count):
        def body(wq_block, wk_block, wv_block, k_block, v_block, context_block):
            queries, keys, values = [project_block(normed_ref, w) for w in (wq_block, wk_block, wv_block)]
            k_block[...] = keys
            v_block[...] = values
            attend_heads(queries, [keys], [values], head_dim, context_block)

        out_spec = pl.BlockSpec((half, group), lambda n: (0, n + first))
        pltpu.emit_pipeline(
            body, grid=(count,), in_specs=[weight_spec_at(model_dim, group, first)] * 3, out_specs=[out_spec] * 3,
        )(wq_ref, wk_ref, wv_ref, k_ref, v_ref, context_ref.at[half_rows(0)])

    third = groups // 3
    head_groups(0, third)
    base_part(1, near)
    finish(1, 0)
    finish(1, 1)
    head_groups(third, third)
    for index in range(2, chunks):
        finish(1, index)
    head_groups(2 * third, groups - 2 * third)
    for copy in moved[1]:
        copy.wait_recv()
    already = {id(copy) for copy in moved[0]}
    for copy in copies:
        if id(copy) not in already:
            copy.wait_send()


def exchange(table, own_out, own_resid, gain, w_query, w_key, w_value, head_dim):
    seq, model_dim = own_resid.shape
    hidden = w_query.shape[1]
    half = seq // HALVES
    slots = own_out.shape[0] * own_out.shape[1] // table.shape[0]
    staged = jax.ShapeDtypeStruct((HALVES, half, model_dim), jnp.float32)
    out_shape = [
        jax.ShapeDtypeStruct((seq, model_dim), jnp.bfloat16),
        jax.ShapeDtypeStruct((half, hidden), jnp.bfloat16),
        jax.ShapeDtypeStruct((half, hidden), jnp.bfloat16),
        jax.ShapeDtypeStruct((seq, hidden), jnp.bfloat16),
        staged, staged, staged,
    ]
    chunks = model_dim // SEND_COLS
    n_copies = 4 + 2 + 2 * HALVES * chunks
    outs = pl.pallas_call(
        functools.partial(exchange_kernel, head_dim),
        out_shape=out_shape,
        in_specs=[VMEM_SPEC, ANY_SPEC, ANY_SPEC, VMEM_SPEC, ANY_SPEC, ANY_SPEC, ANY_SPEC],
        out_specs=[ANY_SPEC] * len(out_shape),
        scratch_shapes=[
            pltpu.VMEM((2, 3 * half, slots), jnp.bfloat16),
            pltpu.VMEM((half, model_dim), jnp.float32),
            pltpu.VMEM((half, model_dim), jnp.float32),
            pltpu.VMEM((HALVES, half, model_dim), jnp.float32),
            pltpu.VMEM((half, model_dim), jnp.float32),
            pltpu.VMEM((half, model_dim), jnp.bfloat16),
            pltpu.VMEM((half, model_dim), jnp.bfloat16),
            pltpu.VMEM((half, model_dim), jnp.bfloat16),
            pltpu.SemaphoreType.DMA,
            pltpu.SemaphoreType.DMA((n_copies,)),
            pltpu.SemaphoreType.DMA((n_copies,)),
        ],
        compiler_params=pltpu.CompilerParams(vmem_limit_bytes=VMEM_LIMIT, collective_id=0, has_side_effects=True),
        name="exchange",
    )(table, own_out, own_resid, gain, w_query, w_key, w_value)
    return outs[:4]


def second_half_kernel(head_dim, gain_ref, x_ref, wq_ref, wk_ref, wv_ref, k_ref, v_ref, held_ref, context_ref, normed_ref):
    del held_ref
    half, model_dim = x_ref.shape
    normalise(x_ref, gain_ref, normed_ref)
    group = HEAD_GROUP * head_dim
    groups = k_ref.shape[1] // group

    def body(wq_block, wk_block, wv_block, k_block, v_block, context_block):
        queries, keys, values = [project_block(normed_ref, w) for w in (wq_block, wk_block, wv_block)]
        attend_heads(queries, [k_block[...], keys], [v_block[...], values], head_dim, context_block)

    spec = pl.BlockSpec((half, group), lambda n: (0, n))
    pltpu.emit_pipeline(
        body, grid=(groups,), in_specs=[weight_spec_at(model_dim, group, 0)] * 3 + [spec] * 2, out_specs=[spec],
    )(wq_ref, wk_ref, wv_ref, k_ref, v_ref, context_ref.at[pl.ds(half, half)])


def second_half(arrived, gain, w_query, w_key, w_value, keys, values, context, head_dim):
    seq, model_dim = arrived.shape
    hidden = w_query.shape[1]
    half = seq // HALVES
    return pl.pallas_call(
        functools.partial(second_half_kernel, head_dim),
        out_shape=jax.ShapeDtypeStruct(context.shape, context.dtype),
        grid=(1,),
        in_specs=[pl.BlockSpec(gain.shape, lambda n: (0, 0)), pl.BlockSpec((half, model_dim), lambda n: (1, 0))] + [ANY_SPEC] * 6,
        out_specs=ANY_SPEC,
        input_output_aliases={7: 0},
        scratch_shapes=[pltpu.VMEM((half, model_dim), jnp.bfloat16)],
        compiler_params=pltpu.CompilerParams(vmem_limit_bytes=VMEM_LIMIT, dimension_semantics=("arbitrary",)),
        cost_estimate=pl.CostEstimate(flops=6 * half * model_dim * hidden, bytes_accessed=6 * model_dim * hidden, transcendentals=0),
        name="second_half",
    )(gain, arrived, w_query, w_key, w_value, keys, values, context)


def solution(mesh):
    ep_size = mesh.shape['ep']
    token_spec = P(('data', 'pp'), None, 'ep', None, None)
    weight_spec = P('pp', None, None)

    def local_step(expert_out, expert_ids, slot_ids, gates, resid, norm_scale, w_query, w_key, w_value, w_out):
        own_out = expert_out[0, 0]
        own_resid = resid[0, 0, 0]
        model_dim = own_out.shape[2]
        slot_dev = own_out.shape[1] // ep_size
        me = lax.axis_index('ep')
        ids, slots, own_gates = expert_ids[0, 0, 0], slot_ids[0, 0, 0], gates[0, 0, 0]
        code = jnp.where(slots >= 0, ids * slot_dev + (slots - me * slot_dev), -1).astype(jnp.float32)
        own_table = jnp.concatenate([code.T, own_gates.T], axis=0)
        table = lax.all_gather(own_table, 'ep').transpose(0, 2, 1)
        gain = norm_scale.reshape(1, model_dim)
        head_count, head_dim = w_out.shape[1], w_out.shape[2]
        weights = (w_query[0], w_key[0], w_value[0])
        arrived, keys, values, context = exchange(table, own_out, own_resid, gain, *weights, head_dim)
        context = second_half(arrived, gain, *weights, keys, values, context, head_dim)
        flat_out = w_out[0].reshape(head_count * head_dim, model_dim)
        proj = jnp.dot(context, flat_out, preferred_element_type=jnp.float32).astype(jnp.bfloat16)
        result = (arrived.astype(jnp.float32) + proj.astype(jnp.float32)).astype(jnp.bfloat16)
        return result[None, None, None]

    return jax.shard_map(local_step, mesh=mesh, in_specs=(token_spec, token_spec, token_spec, token_spec, token_spec, P('pp', None), weight_spec, weight_spec, weight_spec, P('pp', None, None, None)), out_specs=token_spec, check_vma=False)
```

```python
import functools

import jax
import jax.numpy as jnp
from jax import lax
from jax.experimental import pallas as pl
from jax.experimental.pallas import tpu as pltpu
from jax.sharding import PartitionSpec as P

NORM_EPS = 1e-6
LANES = 128
VMEM_LIMIT = 62 * 2**20
PART_COLS = 512
SEND_COLS = 1024
HEAD_GROUP = 2
WEIGHT_BUFFERS = 3
HALVES = 2
FILL_ROWS = 32
FILL_STEP = 16
GATE_SLOTS = 3
QUERY_ROWS = 128
LOG2_E = 1.4426950408889634
ANY_SPEC = pl.BlockSpec(memory_space=pl.ANY)
VMEM_SPEC = pl.BlockSpec(memory_space=pltpu.VMEM)


def fill_gate_block(table_ref, first_row, first_code, terms_ref, block):
    rows = terms_ref.shape[0] // 3
    slots = terms_ref.shape[1]
    top_k = table_ref.shape[1] // 2
    lane_ids = lax.broadcasted_iota(jnp.int32, (FILL_STEP, LANES), 1).astype(jnp.float32)
    for first in range(0, FILL_ROWS, FILL_STEP):
        begin = block * FILL_ROWS + first
        table = table_ref[pl.ds(pl.multiple_of(first_row + begin, FILL_STEP), FILL_STEP), :]
        codes = [jnp.broadcast_to(table[:, j:j + 1] - first_code, (FILL_STEP, LANES)) for j in range(top_k)]
        gates = [jnp.broadcast_to(table[:, top_k + j:top_k + j + 1], (FILL_STEP, LANES)) for j in range(top_k)]
        for tile in range(slots // LANES):
            here = lane_ids + float(tile * LANES)
            gate = jnp.zeros((FILL_STEP, LANES), jnp.float32)
            for j in range(top_k):
                gate = jnp.where(codes[j] == here, gates[j], gate)
            high = gate.astype(jnp.bfloat16)
            rest = gate - high.astype(jnp.float32)
            middle = rest.astype(jnp.bfloat16)
            low = (rest - middle.astype(jnp.float32)).astype(jnp.bfloat16)
            for k, term in enumerate((high, middle, low)):
                at = pl.ds(pl.multiple_of(k * rows + begin, FILL_STEP), FILL_STEP)
                terms_ref[at, tile * LANES:(tile + 1) * LANES] = term


def normalise(x_ref, gain_ref, normed_ref):
    for first in range(0, x_ref.shape[0], 64):
        x_float = x_ref[first:first + 64].astype(jnp.float32)
        inv_rms = lax.rsqrt(jnp.mean(jnp.square(x_float), axis=-1, keepdims=True) + NORM_EPS)
        normed_ref[first:first + 64] = (x_float * inv_rms * gain_ref[...]).astype(jnp.bfloat16)


def attend_heads(q_ref, key_refs, value_refs, head_dim, out_ref):
    rows = q_ref.shape[0]
    scale = head_dim ** -0.5 * LOG2_E
    q_pos = lax.broadcasted_iota(jnp.int32, (QUERY_ROWS, QUERY_ROWS), 0)
    k_pos = lax.broadcasted_iota(jnp.int32, (QUERY_ROWS, QUERY_ROWS), 1)
    causal = q_pos >= k_pos
    for first in range(0, q_ref.shape[1], head_dim):
        cols = slice(first, first + head_dim)
        for start in range(0, rows, QUERY_ROWS):
            here = slice(start, start + QUERY_ROWS)
            query = q_ref[here, cols]
            spans = [(k, v, 0, rows) for k, v in zip(key_refs[:-1], value_refs[:-1])]
            if start > 0:
                spans.append((key_refs[-1], value_refs[-1], 0, start))
            spans.append((key_refs[-1], value_refs[-1], start, start + QUERY_ROWS))
            scores = [
                lax.dot_general(query, k[lo:hi, cols], (((1,), (1,)), ((), ())), preferred_element_type=jnp.float32) * scale
                for k, _, lo, hi in spans
            ]
            scores[-1] = jnp.where(causal, scores[-1], -jnp.inf)
            top = scores[0].max(axis=-1, keepdims=True)
            for part in scores[1:]:
                top = jnp.maximum(top, part.max(axis=-1, keepdims=True))
            weights = [jnp.exp2(part - top) for part in scores]
            total = weights[0].sum(axis=-1, keepdims=True)
            for part in weights[1:]:
                total = total + part.sum(axis=-1, keepdims=True)
            inverse = 1.0 / total
            mixed = jnp.zeros((QUERY_ROWS, head_dim), jnp.float32)
            for part, (_, v, lo, hi) in zip(weights, spans):
                mixed = mixed + jnp.dot((part * inverse).astype(jnp.bfloat16), v[lo:hi, cols], preferred_element_type=jnp.float32)
            out_ref[here, cols] = mixed.astype(jnp.bfloat16)


def project_block(normed_ref, w_ref):
    return jnp.dot(normed_ref[...], w_ref[...], preferred_element_type=jnp.float32).astype(jnp.bfloat16)


def weight_spec_at(model_dim, cols, first):
    return pl.BlockSpec((model_dim, cols), lambda n: (0, n + first), pipeline_mode=pl.Buffered(WEIGHT_BUFFERS))


def exchange_kernel(head_dim, table_ref, out_rows_ref, resid_ref, gain_ref, wq_ref, wk_ref, wv_ref,
                    arrived_ref, k_ref, v_ref, context_ref, pair_out_ref, cross_out_ref, near_out_ref,
                    terms_0_ref, terms_1_ref, terms_2_ref, pair_in_ref, near_in_ref, cross_in_ref, base_ref, combined_ref, x_ref, normed_ref,
                    q_held_ref, k_held_ref, v_held_ref, load_sem, send_sems, recv_sems):
    me = lax.axis_index('ep')
    stage = lax.axis_index('pp')
    seq, model_dim = resid_ref.shape
    half = seq // HALVES
    experts = out_rows_ref.shape[0]
    slot_dev = out_rows_ref.shape[1] // table_ref.shape[0]
    first_code = (me * (experts * slot_dev)).astype(jnp.float32)
    partner, across, diagonal = me ^ 1, me ^ 2, me ^ 3
    next_stage = 1 - stage

    barrier = pltpu.get_barrier_semaphore()
    pl.semaphore_signal(barrier, inc=1, device_id={'ep': partner}, device_id_type=pl.DeviceIdType.MESH)
    pl.semaphore_signal(barrier, inc=1, device_id={'ep': across}, device_id_type=pl.DeviceIdType.MESH)
    pl.semaphore_signal(barrier, inc=1, device_id={'pp': next_stage}, device_id_type=pl.DeviceIdType.MESH)
    pl.semaphore_wait(barrier, 3)

    copies = []
    terms_refs = (terms_0_ref, terms_1_ref, terms_2_ref)

    def send(src_ref, dst_ref, target):
        index = len(copies)
        copy = pltpu.make_async_remote_copy(
            src_ref=src_ref, dst_ref=dst_ref, send_sem=send_sems.at[index], recv_sem=recv_sems.at[index],
            device_id=target, device_id_type=pl.DeviceIdType.MESH)
        copy.start()
        copies.append(copy)
        return copy

    owners = (diagonal, across, partner, me) * HALVES
    fill_blocks = half // FILL_ROWS

    def fill(job, block):
        fill_gate_block(table_ref.at[owners[job]], job // 4 * half, first_code, terms_refs[job % GATE_SLOTS], block)

    def partial_sums(job, first, cols, dst_ref=None, extra_ref=None, resid=None, keep_ref=None, ahead=None):
        steps, begin = cols // PART_COLS, first // PART_COLS
        owner = owners[job]

        def body(block_ref, *refs):
            block = block_ref[...].reshape(experts * slot_dev, PART_COLS)
            sums = jnp.dot(terms_refs[job % GATE_SLOTS][...], block, preferred_element_type=jnp.float32)
            total = sums[:half] + (sums[half:2 * half] + sums[2 * half:])
            at = pl.ds(pl.multiple_of((pl.program_id(0) + begin) * PART_COLS, PART_COLS), PART_COLS)
            if extra_ref is not None:
                total = total + extra_ref[:, at]
            if resid is not None:
                total = refs[0][...].astype(jnp.float32) + total
            if keep_ref is not None:
                keep_ref[:, at] = total
            else:
                refs[-1][...] = total
            if ahead is not None:
                per_step = fill_blocks // steps
                for i in range(per_step):
                    fill(ahead, pl.program_id(0) * per_step + i)

        col_spec = pl.BlockSpec((half, PART_COLS), lambda n: (0, n + begin))
        in_specs = [pl.BlockSpec((experts, slot_dev, PART_COLS), lambda n: (0, owner, n + begin))]
        operands = [out_rows_ref]
        if resid is not None:
            in_specs.append(col_spec)
            operands.append(resid)
        if keep_ref is None:
            pltpu.emit_pipeline(body, grid=(steps,), in_specs=in_specs, out_specs=[col_spec])(*operands, dst_ref)
        else:
            pltpu.emit_pipeline(body, grid=(steps,), in_specs=in_specs)(*operands)

    def col_span(first, cols):
        return (slice(None), pl.ds(first, cols))

    def half_rows(part):
        return pl.ds(part * half, half)

    def pair_part(part, first, cols, ahead=None):
        source = pair_out_ref.at[part]
        partial_sums(4 * part, first, cols, source, ahead=ahead)
        span = col_span(first, cols)
        return send(source.at[span], pair_in_ref.at[span], {'ep': partner})

    def cross_part(part, first, cols, pair, ahead=None):
        pair.wait_recv()
        source = cross_out_ref.at[part]
        partial_sums(4 * part + 1, first, cols, source, extra_ref=pair_in_ref, ahead=ahead)
        for at in range(first, first + cols, SEND_COLS):
            span = col_span(at, SEND_COLS)
            crossed[part].append(send(source.at[span], cross_in_ref.at[part].at[span], {'ep': across}))

    def near_part(part, ahead=None):
        source = near_out_ref.at[part]
        partial_sums(4 * part + 2, 0, model_dim, source, ahead=ahead)
        return send(source, near_in_ref, {'ep': partner})

    def base_part(part, near, ahead=None):
        near.wait_recv()
        partial_sums(4 * part + 3, 0, model_dim, extra_ref=near_in_ref, resid=resid_ref.at[half_rows(part)], keep_ref=base_ref, ahead=ahead)

    def finish(part, index):
        if part > 0:
            moved[part - 1][index].wait_send()
        crossed[part][index].wait_recv()
        span = col_span(index * SEND_COLS, SEND_COLS)
        combined_ref[span] = (base_ref[span] + cross_in_ref[(part,) + span]).astype(jnp.bfloat16)
        target = arrived_ref.at[half_rows(part), pl.ds(index * SEND_COLS, SEND_COLS)]
        moved[part].append(send(combined_ref.at[span], target, {'pp': next_stage}))

    crossed = [[], []]
    moved = [[], []]
    chunks = model_dim // SEND_COLS
    one, rest = SEND_COLS, model_dim - 2 * SEND_COLS

    @pl.loop(0, fill_blocks)
    def _(block):
        fill(0, block)

    pair_a = pair_part(0, 0, one, ahead=1)
    cross_part(0, 0, one, pair_a)
    pair_b = pair_part(0, one, one)
    pair_c = pair_part(0, 2 * one, rest, ahead=2)
    cross_part(0, one, one, pair_b)
    cross_part(0, 2 * one, rest, pair_c, ahead=3)
    near = near_part(0, ahead=4)
    base_part(0, near, ahead=5)
    finish(0, 0)
    finish(0, 1)
    pair_d = pair_part(1, 0, model_dim, ahead=6)
    finish(0, 2)
    cross_part(1, 0, model_dim, pair_d, ahead=7)
    for index in range(3, chunks):
        finish(0, index)
    near = near_part(1)

    for copy in moved[0]:
        copy.wait_recv()
    load = pltpu.make_async_copy(arrived_ref.at[half_rows(0)], x_ref, load_sem)
    load.start()
    load.wait()
    normalise(x_ref, gain_ref, normed_ref)

    group = HEAD_GROUP * head_dim
    groups = k_ref.shape[1] // group

    attend_scratch = (q_held_ref, [k_held_ref], [v_held_ref])

    def head_groups(first, count):
        def body(wq_block, wk_block, wv_block, k_block, v_block, context_block):
            attend_heads(*attend_scratch, head_dim, context_block)
            keys, values = project_block(normed_ref, wk_block), project_block(normed_ref, wv_block)
            k_block[...] = keys
            v_block[...] = values
            q_held_ref[...] = project_block(normed_ref, wq_block)
            k_held_ref[...] = keys
            v_held_ref[...] = values

        out_spec = pl.BlockSpec((half, group), lambda n: (0, n + first))
        late_spec = pl.BlockSpec((half, group), lambda n: (0, jnp.maximum(n + first - 1, 0)))
        pltpu.emit_pipeline(
            body, grid=(count,), in_specs=[weight_spec_at(model_dim, group, first)] * 3, out_specs=[out_spec, out_spec, late_spec],
        )(wq_ref, wk_ref, wv_ref, k_ref, v_ref, context_ref.at[half_rows(0)])

    def last_group(context_block):
        attend_heads(*attend_scratch, head_dim, context_block)

    for ref in (q_held_ref, k_held_ref, v_held_ref):
        ref[...] = jnp.zeros_like(ref)
    third = groups // 3
    head_groups(0, third)
    base_part(1, near)
    finish(1, 0)
    finish(1, 1)
    head_groups(third, third)
    for index in range(2, chunks):
        finish(1, index)
    head_groups(2 * third, groups - 2 * third)
    pltpu.emit_pipeline(last_group, grid=(1,), out_specs=[pl.BlockSpec((half, group), lambda n: (0, groups - 1))])(
        context_ref.at[half_rows(0)])
    for copy in moved[1]:
        copy.wait_recv()
    already = {id(copy) for copy in moved[0]}
    for copy in copies:
        if id(copy) not in already:
            copy.wait_send()


def exchange(table, own_out, own_resid, gain, w_query, w_key, w_value, head_dim):
    seq, model_dim = own_resid.shape
    hidden = w_query.shape[1]
    half = seq // HALVES
    slots = own_out.shape[0] * own_out.shape[1] // table.shape[0]
    staged = jax.ShapeDtypeStruct((HALVES, half, model_dim), jnp.float32)
    out_shape = [
        jax.ShapeDtypeStruct((seq, model_dim), jnp.bfloat16),
        jax.ShapeDtypeStruct((half, hidden), jnp.bfloat16),
        jax.ShapeDtypeStruct((half, hidden), jnp.bfloat16),
        jax.ShapeDtypeStruct((seq, hidden), jnp.bfloat16),
        staged, staged, staged,
    ]
    chunks = model_dim // SEND_COLS
    n_copies = 4 + 2 + 2 * HALVES * chunks
    outs = pl.pallas_call(
        functools.partial(exchange_kernel, head_dim),
        out_shape=out_shape,
        in_specs=[VMEM_SPEC, ANY_SPEC, ANY_SPEC, VMEM_SPEC, ANY_SPEC, ANY_SPEC, ANY_SPEC],
        out_specs=[ANY_SPEC] * len(out_shape),
        scratch_shapes=[
            *[pltpu.VMEM((3 * half, slots), jnp.bfloat16)] * GATE_SLOTS,
            pltpu.VMEM((half, model_dim), jnp.float32),
            pltpu.VMEM((half, model_dim), jnp.float32),
            pltpu.VMEM((HALVES, half, model_dim), jnp.float32),
            pltpu.VMEM((half, model_dim), jnp.float32),
            pltpu.VMEM((half, model_dim), jnp.bfloat16),
            pltpu.VMEM((half, model_dim), jnp.bfloat16),
            pltpu.VMEM((half, model_dim), jnp.bfloat16),
            *[pltpu.VMEM((half, HEAD_GROUP * head_dim), jnp.bfloat16)] * 3,
            pltpu.SemaphoreType.DMA,
            pltpu.SemaphoreType.DMA((n_copies,)),
            pltpu.SemaphoreType.DMA((n_copies,)),
        ],
        compiler_params=pltpu.CompilerParams(vmem_limit_bytes=VMEM_LIMIT, collective_id=0, has_side_effects=True),
        name="exchange",
    )(table, own_out, own_resid, gain, w_query, w_key, w_value)
    return outs[:4]


def second_half_kernel(head_dim, gain_ref, x_ref, wq_ref, wk_ref, wv_ref, k_ref, v_ref, held_ref, context_ref,
                       normed_ref, q_held_ref, k_held_ref, v_held_ref):
    del held_ref
    half, model_dim = x_ref.shape
    normalise(x_ref, gain_ref, normed_ref)
    group = HEAD_GROUP * head_dim
    groups = k_ref.shape[1] // group
    for ref in (q_held_ref, k_held_ref, v_held_ref):
        ref[...] = jnp.zeros_like(ref)

    def attend_before(k_block, v_block, context_block):
        attend_heads(q_held_ref, [k_block, k_held_ref], [v_block, v_held_ref], head_dim, context_block)

    def body(wq_block, wk_block, wv_block, k_block, v_block, context_block):
        attend_before(k_block, v_block, context_block)
        keys, values = project_block(normed_ref, wk_block), project_block(normed_ref, wv_block)
        q_held_ref[...] = project_block(normed_ref, wq_block)
        k_held_ref[...] = keys
        v_held_ref[...] = values

    late_spec = pl.BlockSpec((half, group), lambda n: (0, jnp.maximum(n - 1, 0)))
    last_spec = pl.BlockSpec((half, group), lambda n: (0, groups - 1))
    target = context_ref.at[pl.ds(half, half)]
    pltpu.emit_pipeline(
        body, grid=(groups,), in_specs=[weight_spec_at(model_dim, group, 0)] * 3 + [late_spec] * 2, out_specs=[late_spec],
    )(wq_ref, wk_ref, wv_ref, k_ref, v_ref, target)
    pltpu.emit_pipeline(attend_before, grid=(1,), in_specs=[last_spec] * 2, out_specs=[last_spec])(k_ref, v_ref, target)


def second_half(arrived, gain, w_query, w_key, w_value, keys, values, context, head_dim):
    seq, model_dim = arrived.shape
    hidden = w_query.shape[1]
    half = seq // HALVES
    return pl.pallas_call(
        functools.partial(second_half_kernel, head_dim),
        out_shape=jax.ShapeDtypeStruct(context.shape, context.dtype),
        grid=(1,),
        in_specs=[pl.BlockSpec(gain.shape, lambda n: (0, 0)), pl.BlockSpec((half, model_dim), lambda n: (1, 0))] + [ANY_SPEC] * 6,
        out_specs=ANY_SPEC,
        input_output_aliases={7: 0},
        scratch_shapes=[pltpu.VMEM((half, model_dim), jnp.bfloat16)] + [pltpu.VMEM((half, HEAD_GROUP * head_dim), jnp.bfloat16)] * 3,
        compiler_params=pltpu.CompilerParams(vmem_limit_bytes=VMEM_LIMIT, dimension_semantics=("arbitrary",)),
        cost_estimate=pl.CostEstimate(flops=6 * half * model_dim * hidden, bytes_accessed=6 * model_dim * hidden, transcendentals=0),
        name="second_half",
    )(gain, arrived, w_query, w_key, w_value, keys, values, context)


def solution(mesh):
    ep_size = mesh.shape['ep']
    token_spec = P(('data', 'pp'), None, 'ep', None, None)
    weight_spec = P('pp', None, None)

    def local_step(expert_out, expert_ids, slot_ids, gates, resid, norm_scale, w_query, w_key, w_value, w_out):
        own_out = expert_out[0, 0]
        own_resid = resid[0, 0, 0]
        model_dim = own_out.shape[2]
        slot_dev = own_out.shape[1] // ep_size
        me = lax.axis_index('ep')
        ids, slots, own_gates = expert_ids[0, 0, 0], slot_ids[0, 0, 0], gates[0, 0, 0]
        code = jnp.where(slots >= 0, ids * slot_dev + (slots - me * slot_dev), -1).astype(jnp.float32)
        own_table = jnp.concatenate([code.T, own_gates.T], axis=0)
        table = lax.all_gather(own_table, 'ep').transpose(0, 2, 1)
        gain = norm_scale.reshape(1, model_dim)
        head_count, head_dim = w_out.shape[1], w_out.shape[2]
        weights = (w_query[0], w_key[0], w_value[0])
        arrived, keys, values, context = exchange(table, own_out, own_resid, gain, *weights, head_dim)
        context = second_half(arrived, gain, *weights, keys, values, context, head_dim)
        flat_out = w_out[0].reshape(head_count * head_dim, model_dim)
        proj = jnp.dot(context, flat_out, preferred_element_type=jnp.float32).astype(jnp.bfloat16)
        result = (arrived.astype(jnp.float32) + proj.astype(jnp.float32)).astype(jnp.bfloat16)
        return result[None, None, None]

    return jax.shard_map(local_step, mesh=mesh, in_specs=(token_spec, token_spec, token_spec, token_spec, token_spec, P('pp', None), weight_spec, weight_spec, weight_spec, P('pp', None, None, None)), out_specs=token_spec, check_vma=False)
```

```python
import functools

import jax
import jax.numpy as jnp
from jax import lax
from jax.experimental import pallas as pl
from jax.experimental.pallas import tpu as pltpu
from jax.sharding import PartitionSpec as P

NORM_EPS = 1e-6
LANES = 128
VMEM_LIMIT = 62 * 2**20
PART_COLS = 512
SEND_COLS = 1024
HEAD_GROUP = 2
WEIGHT_BUFFERS = 3
HALVES = 2
FILL_ROWS = 32
FILL_STEP = 16
GATE_SLOTS = 3
LOG2_E = 1.4426950408889634
ANY_SPEC = pl.BlockSpec(memory_space=pl.ANY)
VMEM_SPEC = pl.BlockSpec(memory_space=pltpu.VMEM)


def fill_gate_block(table_ref, first_row, first_code, terms_ref, block):
    rows = terms_ref.shape[0] // 3
    slots = terms_ref.shape[1]
    top_k = table_ref.shape[1] // 2
    lane_ids = lax.broadcasted_iota(jnp.int32, (FILL_STEP, LANES), 1).astype(jnp.float32)
    for first in range(0, FILL_ROWS, FILL_STEP):
        begin = block * FILL_ROWS + first
        table = table_ref[pl.ds(pl.multiple_of(first_row + begin, FILL_STEP), FILL_STEP), :]
        codes = [jnp.broadcast_to(table[:, j:j + 1] - first_code, (FILL_STEP, LANES)) for j in range(top_k)]
        gates = [jnp.broadcast_to(table[:, top_k + j:top_k + j + 1], (FILL_STEP, LANES)) for j in range(top_k)]
        for tile in range(slots // LANES):
            here = lane_ids + float(tile * LANES)
            gate = jnp.zeros((FILL_STEP, LANES), jnp.float32)
            for j in range(top_k):
                gate = jnp.where(codes[j] == here, gates[j], gate)
            high = gate.astype(jnp.bfloat16)
            rest = gate - high.astype(jnp.float32)
            middle = rest.astype(jnp.bfloat16)
            low = (rest - middle.astype(jnp.float32)).astype(jnp.bfloat16)
            for k, term in enumerate((high, middle, low)):
                at = pl.ds(pl.multiple_of(k * rows + begin, FILL_STEP), FILL_STEP)
                terms_ref[at, tile * LANES:(tile + 1) * LANES] = term


def normalise(x_ref, gain_ref, normed_ref):
    for first in range(0, x_ref.shape[0], 64):
        x_float = x_ref[first:first + 64].astype(jnp.float32)
        inv_rms = lax.rsqrt(jnp.mean(jnp.square(x_float), axis=-1, keepdims=True) + NORM_EPS)
        normed_ref[first:first + 64] = (x_float * inv_rms * gain_ref[...]).astype(jnp.bfloat16)


def head_scores(q_ref, key_refs, head_dim):
    return [
        [
            lax.dot_general(k[:, c:c + head_dim], q_ref[:, c:c + head_dim], (((1,), (1,)), ((), ())), preferred_element_type=jnp.float32)
            for k in key_refs
        ]
        for c in range(0, q_ref.shape[1], head_dim)
    ]


def head_context(all_scores, value_refs, head_dim, out_ref):
    rows = out_ref.shape[0]
    scale = head_dim ** -0.5 * LOG2_E
    k_pos = lax.broadcasted_iota(jnp.int32, (rows, rows), 0)
    q_pos = lax.broadcasted_iota(jnp.int32, (rows, rows), 1)
    causal = q_pos >= k_pos
    probs = []
    for scores in all_scores:
        scores = [part * scale for part in scores]
        scores[-1] = jnp.where(causal, scores[-1], -jnp.inf)
        top = scores[0].max(axis=0, keepdims=True)
        for part in scores[1:]:
            top = jnp.maximum(top, part.max(axis=0, keepdims=True))
        weights = [jnp.exp2(part - top) for part in scores]
        total = weights[0].sum(axis=0, keepdims=True)
        for part in weights[1:]:
            total = total + part.sum(axis=0, keepdims=True)
        inverse = 1.0 / total
        probs.append([(part * inverse).astype(jnp.bfloat16) for part in weights])
    for h, parts in enumerate(probs):
        cols = slice(h * head_dim, (h + 1) * head_dim)
        mixed = jnp.zeros((rows, head_dim), jnp.float32)
        for part, v in zip(parts, value_refs):
            mixed = mixed + lax.dot_general(part, v[:, cols], (((0,), (0,)), ((), ())), preferred_element_type=jnp.float32)
        out_ref[:, cols] = mixed.astype(jnp.bfloat16)


def attend_heads(q_ref, key_refs, value_refs, head_dim, out_ref):
    head_context(head_scores(q_ref, key_refs, head_dim), value_refs, head_dim, out_ref)


def project_block(normed_ref, w_ref):
    return jnp.dot(normed_ref[...], w_ref[...], preferred_element_type=jnp.float32).astype(jnp.bfloat16)


def weight_spec_at(model_dim, cols, first):
    return pl.BlockSpec((model_dim, cols), lambda n: (0, n + first), pipeline_mode=pl.Buffered(WEIGHT_BUFFERS))


def exchange_kernel(head_dim, table_ref, out_rows_ref, resid_ref, gain_ref, wq_ref, wk_ref, wv_ref,
                    arrived_ref, k_ref, v_ref, context_ref, pair_out_ref, cross_out_ref, near_out_ref,
                    terms_0_ref, terms_1_ref, terms_2_ref, pair_in_ref, near_in_ref, cross_in_ref, base_ref, combined_ref, x_ref, normed_ref,
                    q_held_ref, k_held_ref, v_held_ref, load_sem, send_sems, recv_sems):
    me = lax.axis_index('ep')
    stage = lax.axis_index('pp')
    seq, model_dim = resid_ref.shape
    half = seq // HALVES
    experts = out_rows_ref.shape[0]
    slot_dev = out_rows_ref.shape[1] // table_ref.shape[0]
    first_code = (me * (experts * slot_dev)).astype(jnp.float32)
    partner, across, diagonal = me ^ 1, me ^ 2, me ^ 3
    next_stage = 1 - stage

    barrier = pltpu.get_barrier_semaphore()
    pl.semaphore_signal(barrier, inc=1, device_id={'ep': partner}, device_id_type=pl.DeviceIdType.MESH)
    pl.semaphore_signal(barrier, inc=1, device_id={'ep': across}, device_id_type=pl.DeviceIdType.MESH)
    pl.semaphore_signal(barrier, inc=1, device_id={'pp': next_stage}, device_id_type=pl.DeviceIdType.MESH)
    pl.semaphore_wait(barrier, 3)

    copies = []
    terms_refs = (terms_0_ref, terms_1_ref, terms_2_ref)

    def send(src_ref, dst_ref, target):
        index = len(copies)
        copy = pltpu.make_async_remote_copy(
            src_ref=src_ref, dst_ref=dst_ref, send_sem=send_sems.at[index], recv_sem=recv_sems.at[index],
            device_id=target, device_id_type=pl.DeviceIdType.MESH)
        copy.start()
        copies.append(copy)
        return copy

    owners = (diagonal, across, partner, me) * HALVES
    fill_blocks = half // FILL_ROWS

    def fill(job, block):
        fill_gate_block(table_ref.at[owners[job]], job // 4 * half, first_code, terms_refs[job % GATE_SLOTS], block)

    def partial_sums(job, first, cols, dst_ref=None, extra_ref=None, resid=None, keep_ref=None, ahead=None):
        steps, begin = cols // PART_COLS, first // PART_COLS
        owner = owners[job]

        def body(block_ref, *refs):
            block = block_ref[...].reshape(experts * slot_dev, PART_COLS)
            sums = jnp.dot(terms_refs[job % GATE_SLOTS][...], block, preferred_element_type=jnp.float32)
            total = sums[:half] + (sums[half:2 * half] + sums[2 * half:])
            at = pl.ds(pl.multiple_of((pl.program_id(0) + begin) * PART_COLS, PART_COLS), PART_COLS)
            if extra_ref is not None:
                total = total + extra_ref[:, at]
            if resid is not None:
                total = refs[0][...].astype(jnp.float32) + total
            if keep_ref is not None:
                keep_ref[:, at] = total
            else:
                refs[-1][...] = total
            if ahead is not None:
                per_step = fill_blocks // steps
                for i in range(per_step):
                    fill(ahead, pl.program_id(0) * per_step + i)

        col_spec = pl.BlockSpec((half, PART_COLS), lambda n: (0, n + begin))
        in_specs = [pl.BlockSpec((experts, slot_dev, PART_COLS), lambda n: (0, owner, n + begin))]
        operands = [out_rows_ref]
        if resid is not None:
            in_specs.append(col_spec)
            operands.append(resid)
        if keep_ref is None:
            pltpu.emit_pipeline(body, grid=(steps,), in_specs=in_specs, out_specs=[col_spec])(*operands, dst_ref)
        else:
            pltpu.emit_pipeline(body, grid=(steps,), in_specs=in_specs)(*operands)

    def col_span(first, cols):
        return (slice(None), pl.ds(first, cols))

    def half_rows(part):
        return pl.ds(part * half, half)

    def pair_part(part, first, cols, ahead=None, after=None):
        source = pair_out_ref.at[part]
        partial_sums(4 * part, first, cols, source, ahead=ahead)
        if after is not None:
            after.wait_recv()
        span = col_span(first, cols)
        return send(source.at[span], pair_in_ref.at[span], {'ep': partner})

    def cross_part(part, first, cols, pair, ahead=None):
        pair.wait_recv()
        source = cross_out_ref.at[part]
        partial_sums(4 * part + 1, first, cols, source, extra_ref=pair_in_ref, ahead=ahead)
        for at in range(first, first + cols, SEND_COLS):
            span = col_span(at, SEND_COLS)
            crossed[part].append(send(source.at[span], cross_in_ref.at[part].at[span], {'ep': across}))

    def near_part(part, ahead=None):
        source = near_out_ref.at[part]
        partial_sums(4 * part + 2, 0, model_dim, source, ahead=ahead)
        return send(source, near_in_ref, {'ep': partner})

    def base_part(part, ahead=None):
        partial_sums(4 * part + 3, 0, model_dim, extra_ref=near_in_ref, resid=resid_ref.at[half_rows(part)], keep_ref=base_ref, ahead=ahead)

    def finish(part, index):
        if part > 0:
            moved[part - 1][index].wait_send()
        crossed[part][index].wait_recv()
        span = col_span(index * SEND_COLS, SEND_COLS)
        combined_ref[span] = (base_ref[span] + cross_in_ref[(part,) + span]).astype(jnp.bfloat16)
        target = arrived_ref.at[half_rows(part), pl.ds(index * SEND_COLS, SEND_COLS)]
        moved[part].append(send(combined_ref.at[span], target, {'pp': next_stage}))

    crossed = [[], []]
    moved = [[], []]
    chunks = model_dim // SEND_COLS
    one, rest = SEND_COLS, model_dim - 2 * SEND_COLS

    @pl.loop(0, fill_blocks)
    def _(block):
        fill(0, block)

    pair_a = pair_part(0, 0, one, ahead=1)
    cross_part(0, 0, one, pair_a)
    pair_b = pair_part(0, one, one)
    pair_c = pair_part(0, 2 * one, rest, ahead=2)
    cross_part(0, one, one, pair_b)
    cross_part(0, 2 * one, rest, pair_c, ahead=3)
    near = near_part(0, ahead=4)
    middle = model_dim // 2
    pair_d = pair_part(1, 0, middle, after=near)
    base_part(0, ahead=5)
    finish(0, 0)
    finish(0, 1)
    pair_e = pair_part(1, middle, middle, ahead=6)
    finish(0, 2)
    cross_part(1, 0, middle, pair_d, ahead=7)
    for index in range(3, chunks):
        finish(0, index)
    cross_part(1, middle, middle, pair_e)
    near = near_part(1)

    for copy in moved[0]:
        copy.wait_recv()
    load = pltpu.make_async_copy(arrived_ref.at[half_rows(0)], x_ref, load_sem)
    load.start()
    load.wait()
    normalise(x_ref, gain_ref, normed_ref)

    group = HEAD_GROUP * head_dim
    groups = k_ref.shape[1] // group

    def head_groups(first, count):
        def body(wq_block, wk_block, wv_block, k_block, v_block, context_block):
            scores = head_scores(q_held_ref, [k_held_ref], head_dim)
            queries = project_block(normed_ref, wq_block)
            keys = project_block(normed_ref, wk_block)
            head_context(scores, [v_held_ref], head_dim, context_block)
            values = project_block(normed_ref, wv_block)
            k_block[...] = keys
            v_block[...] = values
            q_held_ref[...] = queries
            k_held_ref[...] = keys
            v_held_ref[...] = values

        out_spec = pl.BlockSpec((half, group), lambda n: (0, n + first))
        late_spec = pl.BlockSpec((half, group), lambda n: (0, jnp.maximum(n + first - 1, 0)))
        pltpu.emit_pipeline(
            body, grid=(count,), in_specs=[weight_spec_at(model_dim, group, first)] * 3, out_specs=[out_spec, out_spec, late_spec],
        )(wq_ref, wk_ref, wv_ref, k_ref, v_ref, context_ref.at[half_rows(0)])

    def last_group(context_block):
        attend_heads(q_held_ref, [k_held_ref], [v_held_ref], head_dim, context_block)

    for ref in (q_held_ref, k_held_ref, v_held_ref):
        ref[...] = jnp.zeros_like(ref)
    third = groups // 3
    head_groups(0, third)
    near.wait_recv()
    base_part(1)
    finish(1, 0)
    finish(1, 1)
    head_groups(third, third)
    for index in range(2, chunks):
        finish(1, index)
    head_groups(2 * third, groups - 2 * third)
    pltpu.emit_pipeline(last_group, grid=(1,), out_specs=[pl.BlockSpec((half, group), lambda n: (0, groups - 1))])(
        context_ref.at[half_rows(0)])
    for copy in moved[1]:
        copy.wait_recv()
    already = {id(copy) for copy in moved[0]}
    for copy in copies:
        if id(copy) not in already:
            copy.wait_send()


def exchange(table, own_out, own_resid, gain, w_query, w_key, w_value, head_dim):
    seq, model_dim = own_resid.shape
    hidden = w_query.shape[1]
    half = seq // HALVES
    slots = own_out.shape[0] * own_out.shape[1] // table.shape[0]
    staged = jax.ShapeDtypeStruct((HALVES, half, model_dim), jnp.float32)
    out_shape = [
        jax.ShapeDtypeStruct((seq, model_dim), jnp.bfloat16),
        jax.ShapeDtypeStruct((half, hidden), jnp.bfloat16),
        jax.ShapeDtypeStruct((half, hidden), jnp.bfloat16),
        jax.ShapeDtypeStruct((seq, hidden), jnp.bfloat16),
        staged, staged, staged,
    ]
    chunks = model_dim // SEND_COLS
    n_copies = 5 + 2 + 2 * HALVES * chunks
    outs = pl.pallas_call(
        functools.partial(exchange_kernel, head_dim),
        out_shape=out_shape,
        in_specs=[VMEM_SPEC, ANY_SPEC, ANY_SPEC, VMEM_SPEC, ANY_SPEC, ANY_SPEC, ANY_SPEC],
        out_specs=[ANY_SPEC] * len(out_shape),
        scratch_shapes=[
            *[pltpu.VMEM((3 * half, slots), jnp.bfloat16)] * GATE_SLOTS,
            pltpu.VMEM((half, model_dim), jnp.float32),
            pltpu.VMEM((half, model_dim), jnp.float32),
            pltpu.VMEM((HALVES, half, model_dim), jnp.float32),
            pltpu.VMEM((half, model_dim), jnp.float32),
            pltpu.VMEM((half, model_dim), jnp.bfloat16),
            pltpu.VMEM((half, model_dim), jnp.bfloat16),
            pltpu.VMEM((half, model_dim), jnp.bfloat16),
            *[pltpu.VMEM((half, HEAD_GROUP * head_dim), jnp.bfloat16)] * 3,
            pltpu.SemaphoreType.DMA,
            pltpu.SemaphoreType.DMA((n_copies,)),
            pltpu.SemaphoreType.DMA((n_copies,)),
        ],
        compiler_params=pltpu.CompilerParams(vmem_limit_bytes=VMEM_LIMIT, collective_id=0, has_side_effects=True),
        name="exchange",
    )(table, own_out, own_resid, gain, w_query, w_key, w_value)
    return outs[:4]


def second_half_kernel(head_dim, gain_ref, x_ref, wq_ref, wk_ref, wv_ref, k_ref, v_ref, held_ref, context_ref,
                       normed_ref, q_held_ref, k_held_ref, v_held_ref):
    del held_ref
    half, model_dim = x_ref.shape
    normalise(x_ref, gain_ref, normed_ref)
    group = HEAD_GROUP * head_dim
    groups = k_ref.shape[1] // group
    for ref in (q_held_ref, k_held_ref, v_held_ref):
        ref[...] = jnp.zeros_like(ref)

    def attend_before(k_block, v_block, context_block):
        attend_heads(q_held_ref, [k_block, k_held_ref], [v_block, v_held_ref], head_dim, context_block)

    def body(wq_block, wk_block, wv_block, k_block, v_block, context_block):
        scores = head_scores(q_held_ref, [k_block, k_held_ref], head_dim)
        queries = project_block(normed_ref, wq_block)
        keys = project_block(normed_ref, wk_block)
        head_context(scores, [v_block, v_held_ref], head_dim, context_block)
        values = project_block(normed_ref, wv_block)
        q_held_ref[...] = queries
        k_held_ref[...] = keys
        v_held_ref[...] = values

    late_spec = pl.BlockSpec((half, group), lambda n: (0, jnp.maximum(n - 1, 0)))
    last_spec = pl.BlockSpec((half, group), lambda n: (0, groups - 1))
    target = context_ref.at[pl.ds(half, half)]
    pltpu.emit_pipeline(
        body, grid=(groups,), in_specs=[weight_spec_at(model_dim, group, 0)] * 3 + [late_spec] * 2, out_specs=[late_spec],
    )(wq_ref, wk_ref, wv_ref, k_ref, v_ref, target)
    pltpu.emit_pipeline(attend_before, grid=(1,), in_specs=[last_spec] * 2, out_specs=[last_spec])(k_ref, v_ref, target)


def second_half(arrived, gain, w_query, w_key, w_value, keys, values, context, head_dim):
    seq, model_dim = arrived.shape
    hidden = w_query.shape[1]
    half = seq // HALVES
    return pl.pallas_call(
        functools.partial(second_half_kernel, head_dim),
        out_shape=jax.ShapeDtypeStruct(context.shape, context.dtype),
        grid=(1,),
        in_specs=[pl.BlockSpec(gain.shape, lambda n: (0, 0)), pl.BlockSpec((half, model_dim), lambda n: (1, 0))] + [ANY_SPEC] * 6,
        out_specs=ANY_SPEC,
        input_output_aliases={7: 0},
        scratch_shapes=[pltpu.VMEM((half, model_dim), jnp.bfloat16)] + [pltpu.VMEM((half, HEAD_GROUP * head_dim), jnp.bfloat16)] * 3,
        compiler_params=pltpu.CompilerParams(vmem_limit_bytes=VMEM_LIMIT, dimension_semantics=("arbitrary",)),
        cost_estimate=pl.CostEstimate(flops=6 * half * model_dim * hidden, bytes_accessed=6 * model_dim * hidden, transcendentals=0),
        name="second_half",
    )(gain, arrived, w_query, w_key, w_value, keys, values, context)


def solution(mesh):
    ep_size = mesh.shape['ep']
    token_spec = P(('data', 'pp'), None, 'ep', None, None)
    weight_spec = P('pp', None, None)

    def local_step(expert_out, expert_ids, slot_ids, gates, resid, norm_scale, w_query, w_key, w_value, w_out):
        own_out = expert_out[0, 0]
        own_resid = resid[0, 0, 0]
        model_dim = own_out.shape[2]
        slot_dev = own_out.shape[1] // ep_size
        me = lax.axis_index('ep')
        ids, slots, own_gates = expert_ids[0, 0, 0], slot_ids[0, 0, 0], gates[0, 0, 0]
        code = jnp.where(slots >= 0, ids * slot_dev + (slots - me * slot_dev), -1).astype(jnp.float32)
        own_table = jnp.concatenate([code.T, own_gates.T], axis=0)
        table = lax.all_gather(own_table, 'ep').transpose(0, 2, 1)
        gain = norm_scale.reshape(1, model_dim)
        head_count, head_dim = w_out.shape[1], w_out.shape[2]
        weights = (w_query[0], w_key[0], w_value[0])
        arrived, keys, values, context = exchange(table, own_out, own_resid, gain, *weights, head_dim)
        context = second_half(arrived, gain, *weights, keys, values, context, head_dim)
        flat_out = w_out[0].reshape(head_count * head_dim, model_dim)
        proj = jnp.dot(context, flat_out, preferred_element_type=jnp.float32).astype(jnp.bfloat16)
        result = (arrived.astype(jnp.float32) + proj.astype(jnp.float32)).astype(jnp.bfloat16)
        return result[None, None, None]

    return jax.shard_map(local_step, mesh=mesh, in_specs=(token_spec, token_spec, token_spec, token_spec, token_spec, P('pp', None), weight_spec, weight_spec, weight_spec, P('pp', None, None, None)), out_specs=token_spec, check_vma=False)
```

```python
import functools

import jax
import jax.numpy as jnp
from jax import lax
from jax.experimental import pallas as pl
from jax.experimental.pallas import tpu as pltpu
from jax.sharding import PartitionSpec as P

NORM_EPS = 1e-6
LANES = 128
VMEM_LIMIT = 62 * 2**20
PART_COLS = 512
SEND_COLS = 1024
HEAD_GROUP = 4
HALVES = 2
FILL_ROWS = 32
FILL_STEP = 16
GATE_SLOTS = 3
LOG2_E = 1.4426950408889634
ANY_SPEC = pl.BlockSpec(memory_space=pl.ANY)
VMEM_SPEC = pl.BlockSpec(memory_space=pltpu.VMEM)


def fill_gate_block(table_ref, first_row, first_code, terms_ref, block):
    rows = terms_ref.shape[0] // 3
    slots = terms_ref.shape[1]
    top_k = table_ref.shape[1] // 2
    lane_ids = lax.broadcasted_iota(jnp.int32, (FILL_STEP, LANES), 1).astype(jnp.float32)
    for first in range(0, FILL_ROWS, FILL_STEP):
        begin = block * FILL_ROWS + first
        table = table_ref[pl.ds(pl.multiple_of(first_row + begin, FILL_STEP), FILL_STEP), :]
        codes = [jnp.broadcast_to(table[:, j:j + 1] - first_code, (FILL_STEP, LANES)) for j in range(top_k)]
        gates = [jnp.broadcast_to(table[:, top_k + j:top_k + j + 1], (FILL_STEP, LANES)) for j in range(top_k)]
        for tile in range(slots // LANES):
            here = lane_ids + float(tile * LANES)
            gate = jnp.zeros((FILL_STEP, LANES), jnp.float32)
            for j in range(top_k):
                gate = jnp.where(codes[j] == here, gates[j], gate)
            high = gate.astype(jnp.bfloat16)
            rest = gate - high.astype(jnp.float32)
            middle = rest.astype(jnp.bfloat16)
            low = (rest - middle.astype(jnp.float32)).astype(jnp.bfloat16)
            for k, term in enumerate((high, middle, low)):
                at = pl.ds(pl.multiple_of(k * rows + begin, FILL_STEP), FILL_STEP)
                terms_ref[at, tile * LANES:(tile + 1) * LANES] = term


def normalise(x_ref, gain_ref, normed_ref):
    for first in range(0, x_ref.shape[0], 64):
        x_float = x_ref[first:first + 64].astype(jnp.float32)
        inv_rms = lax.rsqrt(jnp.mean(jnp.square(x_float), axis=-1, keepdims=True) + NORM_EPS)
        normed_ref[first:first + 64] = (x_float * inv_rms * gain_ref[...]).astype(jnp.bfloat16)


def head_scores(q_ref, key_refs, head_dim):
    return [
        [
            lax.dot_general(k[:, c:c + head_dim], q_ref[:, c:c + head_dim], (((1,), (1,)), ((), ())), preferred_element_type=jnp.float32)
            for k in key_refs
        ]
        for c in range(0, q_ref.shape[1], head_dim)
    ]


def head_context(all_scores, value_refs, head_dim, out_ref):
    rows = out_ref.shape[0]
    scale = head_dim ** -0.5 * LOG2_E
    k_pos = lax.broadcasted_iota(jnp.int32, (rows, rows), 0)
    q_pos = lax.broadcasted_iota(jnp.int32, (rows, rows), 1)
    causal = q_pos >= k_pos
    probs = []
    for scores in all_scores:
        scores = [part * scale for part in scores]
        scores[-1] = jnp.where(causal, scores[-1], -jnp.inf)
        top = scores[0].max(axis=0, keepdims=True)
        for part in scores[1:]:
            top = jnp.maximum(top, part.max(axis=0, keepdims=True))
        weights = [jnp.exp2(part - top) for part in scores]
        total = weights[0].sum(axis=0, keepdims=True)
        for part in weights[1:]:
            total = total + part.sum(axis=0, keepdims=True)
        inverse = 1.0 / total
        probs.append([(part * inverse).astype(jnp.bfloat16) for part in weights])
    for h, parts in enumerate(probs):
        cols = slice(h * head_dim, (h + 1) * head_dim)
        mixed = jnp.zeros((rows, head_dim), jnp.float32)
        for part, v in zip(parts, value_refs):
            mixed = mixed + lax.dot_general(part, v[:, cols], (((0,), (0,)), ((), ())), preferred_element_type=jnp.float32)
        out_ref[:, cols] = mixed.astype(jnp.bfloat16)


def attend_heads(q_ref, key_refs, value_refs, head_dim, out_ref):
    head_context(head_scores(q_ref, key_refs, head_dim), value_refs, head_dim, out_ref)


def project_block(normed_ref, w_ref):
    return jnp.dot(normed_ref[...], w_ref[...], preferred_element_type=jnp.float32).astype(jnp.bfloat16)


def weight_spec_at(model_dim, cols, first, buffers):
    return pl.BlockSpec((model_dim, cols), lambda n: (0, n + first), pipeline_mode=pl.Buffered(buffers))


class Transfer:
    def __init__(self, make_refs, target, send_sems, recv_sems, index):
        self.parts = (make_refs, target, send_sems, recv_sems, index)

    def describe(self):
        make_refs, target, send_sems, recv_sems, index = self.parts
        src_ref, dst_ref = make_refs()
        return pltpu.make_async_remote_copy(
            src_ref=src_ref, dst_ref=dst_ref, send_sem=send_sems.at[index], recv_sem=recv_sems.at[index],
            device_id=target, device_id_type=pl.DeviceIdType.MESH)

    def wait_send(self):
        self.describe().wait_send()

    def wait_recv(self):
        self.describe().wait_recv()


def exchange_kernel(head_dim, table_ref, out_rows_ref, resid_ref, gain_ref, wq_ref, wk_ref, wv_ref,
                    arrived_ref, k_ref, v_ref, context_ref, pair_out_ref, cross_out_ref, near_out_ref,
                    pair_in_ref, near_in_ref, cross_in_ref, base_ref, combined_ref, x_ref, normed_ref,
                    q_held_ref, k_held_ref, v_held_ref, load_sem, send_sems, recv_sems):
    me = lax.axis_index('ep')
    stage = lax.axis_index('pp')
    seq, model_dim = resid_ref.shape
    half = seq // HALVES
    experts = out_rows_ref.shape[0]
    slot_dev = out_rows_ref.shape[1] // table_ref.shape[0]
    first_code = (me * (experts * slot_dev)).astype(jnp.float32)
    partner, across, diagonal = me ^ 1, me ^ 2, me ^ 3
    next_stage = 1 - stage

    barrier = pltpu.get_barrier_semaphore()
    pl.semaphore_signal(barrier, inc=1, device_id={'ep': partner}, device_id_type=pl.DeviceIdType.MESH)
    pl.semaphore_signal(barrier, inc=1, device_id={'ep': across}, device_id_type=pl.DeviceIdType.MESH)
    pl.semaphore_signal(barrier, inc=1, device_id={'pp': next_stage}, device_id_type=pl.DeviceIdType.MESH)
    pl.semaphore_wait(barrier, 3)

    copies = []
    terms_refs = []

    def send(make_refs, target):
        transfer = Transfer(make_refs, target, send_sems, recv_sems, len(copies))
        transfer.describe().start()
        copies.append(transfer)
        return transfer

    owners = (diagonal, across, partner, me) * HALVES
    fill_blocks = half // FILL_ROWS

    def fill(job, block):
        fill_gate_block(table_ref.at[owners[job]], job // 4 * half, first_code, terms_refs[job % GATE_SLOTS], block)

    def partial_sums(job, first, cols, dst_ref=None, extra_ref=None, resid=None, keep_ref=None, ahead=None):
        steps, begin = cols // PART_COLS, first // PART_COLS
        owner = owners[job]

        def body(block_ref, *refs):
            block = block_ref[...].reshape(experts * slot_dev, PART_COLS)
            sums = jnp.dot(terms_refs[job % GATE_SLOTS][...], block, preferred_element_type=jnp.float32)
            total = sums[:half] + (sums[half:2 * half] + sums[2 * half:])
            at = pl.ds(pl.multiple_of((pl.program_id(0) + begin) * PART_COLS, PART_COLS), PART_COLS)
            if extra_ref is not None:
                total = total + extra_ref[:, at]
            if resid is not None:
                total = refs[0][...].astype(jnp.float32) + total
            if keep_ref is not None:
                keep_ref[:, at] = total
            else:
                refs[-1][...] = total
            if ahead is not None:
                per_step = fill_blocks // steps
                for i in range(per_step):
                    fill(ahead, pl.program_id(0) * per_step + i)

        col_spec = pl.BlockSpec((half, PART_COLS), lambda n: (0, n + begin))
        in_specs = [pl.BlockSpec((experts, slot_dev, PART_COLS), lambda n: (0, owner, n + begin))]
        operands = [out_rows_ref]
        if resid is not None:
            in_specs.append(col_spec)
            operands.append(resid)
        if keep_ref is None:
            pltpu.emit_pipeline(body, grid=(steps,), in_specs=in_specs, out_specs=[col_spec])(*operands, dst_ref)
        else:
            pltpu.emit_pipeline(body, grid=(steps,), in_specs=in_specs)(*operands)

    def col_span(first, cols):
        return (slice(None), pl.ds(first, cols))

    def half_rows(part):
        return pl.ds(part * half, half)

    def pair_part(part, first, cols, ahead=None, after=None):
        source = pair_out_ref.at[part]
        partial_sums(4 * part, first, cols, source, ahead=ahead)
        if after is not None:
            after.wait_recv()
        span = col_span(first, cols)
        return send(lambda: (pair_out_ref.at[part].at[span], pair_in_ref.at[span]), {'ep': partner})

    def cross_part(part, first, cols, pair=None, ahead=None):
        if pair is not None:
            pair.wait_recv()
        source = cross_out_ref.at[part]
        partial_sums(4 * part + 1, first, cols, source, extra_ref=pair_in_ref, ahead=ahead)
        for at in range(first, first + cols, SEND_COLS):
            span = col_span(at, SEND_COLS)
            crossed[part].append(send(lambda span=span: (cross_out_ref.at[part].at[span], cross_in_ref.at[part].at[span]), {'ep': across}))

    def near_part(part, ahead=None, after=None):
        source = near_out_ref.at[part]
        partial_sums(4 * part + 2, 0, model_dim, source, ahead=ahead)
        if after is not None:
            after.wait_recv()
        return send(lambda: (near_out_ref.at[part], near_in_ref), {'ep': partner})

    def base_part(part, ahead=None):
        partial_sums(4 * part + 3, 0, model_dim, extra_ref=near_in_ref, resid=resid_ref.at[half_rows(part)], keep_ref=base_ref, ahead=ahead)

    def finish(part, index):
        if part > 0:
            moved[part - 1][index].wait_send()
        crossed[part][index].wait_recv()
        span = col_span(index * SEND_COLS, SEND_COLS)
        combined_ref[span] = (base_ref[span] + cross_in_ref[(part,) + span]).astype(jnp.bfloat16)
        target = (half_rows(part), pl.ds(index * SEND_COLS, SEND_COLS))
        moved[part].append(send(lambda: (combined_ref.at[span], arrived_ref.at[target]), {'pp': next_stage}))

    crossed = [[], []]
    moved = [[], []]
    chunks = model_dim // SEND_COLS
    one, rest = SEND_COLS, model_dim - 2 * SEND_COLS
    middle = model_dim // 2

    def sum_phase(*terms):
        terms_refs.extend(terms)

        @pl.loop(0, fill_blocks)
        def _(block):
            fill(0, block)

        pair_a = pair_part(0, 0, one, ahead=1)
        cross_part(0, 0, one, pair_a)
        pair_b = pair_part(0, one, one)
        pair_c = pair_part(0, 2 * one, rest, ahead=2)
        cross_part(0, one, one, pair_b)
        cross_part(0, 2 * one, rest, pair_c, ahead=3)
        near = near_part(0, ahead=4)
        pair_d = pair_part(1, 0, middle, after=near)
        base_part(0, ahead=5)
        finish(0, 0)
        finish(0, 1)
        pair_e = pair_part(1, middle, middle, ahead=6)
        finish(0, 2)
        cross_part(1, 0, middle, pair_d, ahead=7)
        for index in range(3, chunks):
            finish(0, index)
        near = near_part(1, after=pair_e)
        cross_part(1, middle, middle)
        near.wait_recv()
        base_part(1)

    pl.run_scoped(sum_phase, *[pltpu.VMEM((3 * half, experts * slot_dev), jnp.bfloat16)] * GATE_SLOTS)
    for copy in moved[0]:
        copy.wait_recv()
    load = pltpu.make_async_copy(arrived_ref.at[half_rows(0)], x_ref, load_sem)
    load.start()
    load.wait()
    normalise(x_ref, gain_ref, normed_ref)

    group = HEAD_GROUP * head_dim
    groups = k_ref.shape[1] // group

    def head_groups(first, count):
        def body(wq_block, wk_block, wv_block, k_block, v_block, context_block):
            scores = head_scores(q_held_ref, [k_held_ref], head_dim)
            queries = project_block(normed_ref, wq_block)
            keys = project_block(normed_ref, wk_block)
            head_context(scores, [v_held_ref], head_dim, context_block)
            values = project_block(normed_ref, wv_block)
            k_block[...] = keys
            v_block[...] = values
            q_held_ref[...] = queries
            k_held_ref[...] = keys
            v_held_ref[...] = values

        out_spec = pl.BlockSpec((half, group), lambda n: (0, n + first))
        late_spec = pl.BlockSpec((half, group), lambda n: (0, jnp.maximum(n + first - 1, 0)))
        pltpu.emit_pipeline(
            body, grid=(count,), in_specs=[weight_spec_at(model_dim, group, first, 2)] * 3, out_specs=[out_spec, out_spec, late_spec],
        )(wq_ref, wk_ref, wv_ref, k_ref, v_ref, context_ref.at[half_rows(0)])

    def last_group(context_block):
        attend_heads(q_held_ref, [k_held_ref], [v_held_ref], head_dim, context_block)

    for ref in (q_held_ref, k_held_ref, v_held_ref):
        ref[...] = jnp.zeros_like(ref)
    third = groups // 3
    head_groups(0, third)
    for index in range(chunks - 1):
        finish(1, index)
    head_groups(third, third)
    finish(1, chunks - 1)
    head_groups(2 * third, groups - 2 * third)
    pltpu.emit_pipeline(last_group, grid=(1,), out_specs=[pl.BlockSpec((half, group), lambda n: (0, groups - 1))])(
        context_ref.at[half_rows(0)])
    for copy in moved[1]:
        copy.wait_recv()
    already = {id(copy) for copy in moved[0]}
    for copy in copies:
        if id(copy) not in already:
            copy.wait_send()


def exchange(table, own_out, own_resid, gain, w_query, w_key, w_value, head_dim):
    seq, model_dim = own_resid.shape
    hidden = w_query.shape[1]
    half = seq // HALVES
    staged = jax.ShapeDtypeStruct((HALVES, half, model_dim), jnp.float32)
    out_shape = [
        jax.ShapeDtypeStruct((seq, model_dim), jnp.bfloat16),
        jax.ShapeDtypeStruct((half, hidden), jnp.bfloat16),
        jax.ShapeDtypeStruct((half, hidden), jnp.bfloat16),
        jax.ShapeDtypeStruct((seq, hidden), jnp.bfloat16),
        staged, staged, staged,
    ]
    chunks = model_dim // SEND_COLS
    n_copies = 5 + 2 + 2 * HALVES * chunks
    outs = pl.pallas_call(
        functools.partial(exchange_kernel, head_dim),
        out_shape=out_shape,
        in_specs=[VMEM_SPEC, ANY_SPEC, ANY_SPEC, VMEM_SPEC, ANY_SPEC, ANY_SPEC, ANY_SPEC],
        out_specs=[ANY_SPEC] * len(out_shape),
        scratch_shapes=[
            pltpu.VMEM((half, model_dim), jnp.float32),
            pltpu.VMEM((half, model_dim), jnp.float32),
            pltpu.VMEM((HALVES, half, model_dim), jnp.float32),
            pltpu.VMEM((half, model_dim), jnp.float32),
            pltpu.VMEM((half, model_dim), jnp.bfloat16),
            pltpu.VMEM((half, model_dim), jnp.bfloat16),
            pltpu.VMEM((half, model_dim), jnp.bfloat16),
            *[pltpu.VMEM((half, HEAD_GROUP * head_dim), jnp.bfloat16)] * 3,
            pltpu.SemaphoreType.DMA,
            pltpu.SemaphoreType.DMA((n_copies,)),
            pltpu.SemaphoreType.DMA((n_copies,)),
        ],
        compiler_params=pltpu.CompilerParams(vmem_limit_bytes=VMEM_LIMIT, collective_id=0, has_side_effects=True),
        name="exchange",
    )(table, own_out, own_resid, gain, w_query, w_key, w_value)
    return outs[:4]


def second_half_kernel(head_dim, gain_ref, x_ref, wq_ref, wk_ref, wv_ref, k_ref, v_ref, held_ref, context_ref,
                       normed_ref, q_held_ref, k_held_ref, v_held_ref):
    del held_ref
    half, model_dim = x_ref.shape
    normalise(x_ref, gain_ref, normed_ref)
    group = HEAD_GROUP * head_dim
    groups = k_ref.shape[1] // group
    for ref in (q_held_ref, k_held_ref, v_held_ref):
        ref[...] = jnp.zeros_like(ref)

    def attend_before(k_block, v_block, context_block):
        attend_heads(q_held_ref, [k_block, k_held_ref], [v_block, v_held_ref], head_dim, context_block)

    def body(wq_block, wk_block, wv_block, k_block, v_block, context_block):
        scores = head_scores(q_held_ref, [k_block, k_held_ref], head_dim)
        queries = project_block(normed_ref, wq_block)
        keys = project_block(normed_ref, wk_block)
        head_context(scores, [v_block, v_held_ref], head_dim, context_block)
        values = project_block(normed_ref, wv_block)
        q_held_ref[...] = queries
        k_held_ref[...] = keys
        v_held_ref[...] = values

    late_spec = pl.BlockSpec((half, group), lambda n: (0, jnp.maximum(n - 1, 0)))
    last_spec = pl.BlockSpec((half, group), lambda n: (0, groups - 1))
    target = context_ref.at[pl.ds(half, half)]
    pltpu.emit_pipeline(
        body, grid=(groups,), in_specs=[weight_spec_at(model_dim, group, 0, 3)] * 3 + [late_spec] * 2, out_specs=[late_spec],
    )(wq_ref, wk_ref, wv_ref, k_ref, v_ref, target)
    pltpu.emit_pipeline(attend_before, grid=(1,), in_specs=[last_spec] * 2, out_specs=[last_spec])(k_ref, v_ref, target)


def second_half(arrived, gain, w_query, w_key, w_value, keys, values, context, head_dim):
    seq, model_dim = arrived.shape
    hidden = w_query.shape[1]
    half = seq // HALVES
    return pl.pallas_call(
        functools.partial(second_half_kernel, head_dim),
        out_shape=jax.ShapeDtypeStruct(context.shape, context.dtype),
        grid=(1,),
        in_specs=[pl.BlockSpec(gain.shape, lambda n: (0, 0)), pl.BlockSpec((half, model_dim), lambda n: (1, 0))] + [ANY_SPEC] * 6,
        out_specs=ANY_SPEC,
        input_output_aliases={7: 0},
        scratch_shapes=[pltpu.VMEM((half, model_dim), jnp.bfloat16)] + [pltpu.VMEM((half, HEAD_GROUP * head_dim), jnp.bfloat16)] * 3,
        compiler_params=pltpu.CompilerParams(vmem_limit_bytes=VMEM_LIMIT, dimension_semantics=("arbitrary",)),
        cost_estimate=pl.CostEstimate(flops=6 * half * model_dim * hidden, bytes_accessed=6 * model_dim * hidden, transcendentals=0),
        name="second_half",
    )(gain, arrived, w_query, w_key, w_value, keys, values, context)


def solution(mesh):
    ep_size = mesh.shape['ep']
    token_spec = P(('data', 'pp'), None, 'ep', None, None)
    weight_spec = P('pp', None, None)

    def local_step(expert_out, expert_ids, slot_ids, gates, resid, norm_scale, w_query, w_key, w_value, w_out):
        own_out = expert_out[0, 0]
        own_resid = resid[0, 0, 0]
        model_dim = own_out.shape[2]
        slot_dev = own_out.shape[1] // ep_size
        me = lax.axis_index('ep')
        ids, slots, own_gates = expert_ids[0, 0, 0], slot_ids[0, 0, 0], gates[0, 0, 0]
        code = jnp.where(slots >= 0, ids * slot_dev + (slots - me * slot_dev), -1).astype(jnp.float32)
        own_table = jnp.concatenate([code.T, own_gates.T], axis=0)
        table = lax.all_gather(own_table, 'ep').transpose(0, 2, 1)
        gain = norm_scale.reshape(1, model_dim)
        head_count, head_dim = w_out.shape[1], w_out.shape[2]
        weights = (w_query[0], w_key[0], w_value[0])
        arrived, keys, values, context = exchange(table, own_out, own_resid, gain, *weights, head_dim)
        context = second_half(arrived, gain, *weights, keys, values, context, head_dim)
        flat_out = w_out[0].reshape(head_count * head_dim, model_dim)
        proj = jnp.dot(context, flat_out, preferred_element_type=jnp.float32).astype(jnp.bfloat16)
        result = (arrived.astype(jnp.float32) + proj.astype(jnp.float32)).astype(jnp.bfloat16)
        return result[None, None, None]

    return jax.shard_map(local_step, mesh=mesh, in_specs=(token_spec, token_spec, token_spec, token_spec, token_spec, P('pp', None), weight_spec, weight_spec, weight_spec, P('pp', None, None, None)), out_specs=token_spec, check_vma=False)
```

```python
import functools

import jax
import jax.numpy as jnp
from jax import lax
from jax.experimental import pallas as pl
from jax.experimental.pallas import tpu as pltpu
from jax.sharding import PartitionSpec as P

NORM_EPS = 1e-6
LANES = 128
VMEM_LIMIT = 62 * 2**20
PART_COLS = 512
SEND_COLS = 1024
HEAD_GROUP = 2
LAST_GROUP = 4
WEIGHT_BUFFERS = 3
HALVES = 2
FILL_ROWS = 32
FILL_STEP = 16
GATE_SLOTS = 3
LOG2_E = 1.4426950408889634
ANY_SPEC = pl.BlockSpec(memory_space=pl.ANY)
VMEM_SPEC = pl.BlockSpec(memory_space=pltpu.VMEM)


def fill_gate_block(table_ref, first_row, first_code, terms_ref, block):
    rows = terms_ref.shape[0] // 3
    slots = terms_ref.shape[1]
    top_k = table_ref.shape[1] // 2
    lane_ids = lax.broadcasted_iota(jnp.int32, (FILL_STEP, LANES), 1).astype(jnp.float32)
    for first in range(0, FILL_ROWS, FILL_STEP):
        begin = block * FILL_ROWS + first
        table = table_ref[pl.ds(pl.multiple_of(first_row + begin, FILL_STEP), FILL_STEP), :]
        codes = [jnp.broadcast_to(table[:, j:j + 1] - first_code, (FILL_STEP, LANES)) for j in range(top_k)]
        gates = [jnp.broadcast_to(table[:, top_k + j:top_k + j + 1], (FILL_STEP, LANES)) for j in range(top_k)]
        for tile in range(slots // LANES):
            here = lane_ids + float(tile * LANES)
            gate = jnp.zeros((FILL_STEP, LANES), jnp.float32)
            for j in range(top_k):
                gate = jnp.where(codes[j] == here, gates[j], gate)
            high = gate.astype(jnp.bfloat16)
            rest = gate - high.astype(jnp.float32)
            middle = rest.astype(jnp.bfloat16)
            low = (rest - middle.astype(jnp.float32)).astype(jnp.bfloat16)
            for k, term in enumerate((high, middle, low)):
                at = pl.ds(pl.multiple_of(k * rows + begin, FILL_STEP), FILL_STEP)
                terms_ref[at, tile * LANES:(tile + 1) * LANES] = term


def normalise(x_ref, gain_ref, normed_ref):
    for first in range(0, x_ref.shape[0], 64):
        x_float = x_ref[first:first + 64].astype(jnp.float32)
        inv_rms = lax.rsqrt(jnp.mean(jnp.square(x_float), axis=-1, keepdims=True) + NORM_EPS)
        normed_ref[first:first + 64] = (x_float * inv_rms * gain_ref[...]).astype(jnp.bfloat16)


def head_scores(q_ref, key_refs, head_dim):
    return [
        [
            lax.dot_general(k[:, c:c + head_dim], q_ref[:, c:c + head_dim], (((1,), (1,)), ((), ())), preferred_element_type=jnp.float32)
            for k in key_refs
        ]
        for c in range(0, q_ref.shape[1], head_dim)
    ]


def head_context(all_scores, value_refs, head_dim, out_ref):
    rows = out_ref.shape[0]
    scale = head_dim ** -0.5 * LOG2_E
    k_pos = lax.broadcasted_iota(jnp.int32, (rows, rows), 0)
    q_pos = lax.broadcasted_iota(jnp.int32, (rows, rows), 1)
    causal = q_pos >= k_pos
    probs = []
    for scores in all_scores:
        scores = [part * scale for part in scores]
        scores[-1] = jnp.where(causal, scores[-1], -jnp.inf)
        top = scores[0].max(axis=0, keepdims=True)
        for part in scores[1:]:
            top = jnp.maximum(top, part.max(axis=0, keepdims=True))
        weights = [jnp.exp2(part - top) for part in scores]
        total = weights[0].sum(axis=0, keepdims=True)
        for part in weights[1:]:
            total = total + part.sum(axis=0, keepdims=True)
        inverse = 1.0 / total
        probs.append([(part * inverse).astype(jnp.bfloat16) for part in weights])
    for h, parts in enumerate(probs):
        cols = slice(h * head_dim, (h + 1) * head_dim)
        mixed = jnp.zeros((rows, head_dim), jnp.float32)
        for part, v in zip(parts, value_refs):
            mixed = mixed + lax.dot_general(part, v[:, cols], (((0,), (0,)), ((), ())), preferred_element_type=jnp.float32)
        out_ref[:, cols] = mixed.astype(jnp.bfloat16)


def attend_heads(q_ref, key_refs, value_refs, head_dim, out_ref):
    head_context(head_scores(q_ref, key_refs, head_dim), value_refs, head_dim, out_ref)


def project_block(normed_ref, w_ref):
    return jnp.dot(normed_ref[...], w_ref[...], preferred_element_type=jnp.float32).astype(jnp.bfloat16)


def weight_spec_at(model_dim, cols, first):
    return pl.BlockSpec((model_dim, cols), lambda n: (0, n + first), pipeline_mode=pl.Buffered(WEIGHT_BUFFERS))


def exchange_kernel(head_dim, own_table_ref, out_rows_ref, resid_ref, gain_ref, wq_ref, wk_ref, wv_ref,
                    arrived_ref, k_ref, v_ref, context_ref, pair_out_ref, cross_out_ref, near_out_ref,
                    terms_0_ref, terms_1_ref, terms_2_ref, tables_ref, table_ref, pair_in_ref, near_in_ref, cross_in_ref, base_ref, combined_ref, x_ref, normed_ref,
                    q_held_ref, k_held_ref, v_held_ref, load_sem, send_sems, recv_sems):
    me = lax.axis_index('ep')
    stage = lax.axis_index('pp')
    seq, model_dim = resid_ref.shape
    half = seq // HALVES
    experts = out_rows_ref.shape[0]
    slot_dev = out_rows_ref.shape[1] // table_ref.shape[0]
    first_code = (me * (experts * slot_dev)).astype(jnp.float32)
    partner, across, diagonal = me ^ 1, me ^ 2, me ^ 3
    next_stage = 1 - stage

    barrier = pltpu.get_barrier_semaphore()
    pl.semaphore_signal(barrier, inc=1, device_id={'ep': partner}, device_id_type=pl.DeviceIdType.MESH)
    pl.semaphore_signal(barrier, inc=1, device_id={'ep': across}, device_id_type=pl.DeviceIdType.MESH)
    pl.semaphore_signal(barrier, inc=1, device_id={'ep': diagonal}, device_id_type=pl.DeviceIdType.MESH)
    pl.semaphore_signal(barrier, inc=1, device_id={'pp': next_stage}, device_id_type=pl.DeviceIdType.MESH)
    pl.semaphore_wait(barrier, 4)

    copies = []
    terms_refs = (terms_0_ref, terms_1_ref, terms_2_ref)

    def send(src_ref, dst_ref, target):
        index = len(copies)
        copy = pltpu.make_async_remote_copy(
            src_ref=src_ref, dst_ref=dst_ref, send_sem=send_sems.at[index], recv_sem=recv_sems.at[index],
            device_id=target, device_id_type=pl.DeviceIdType.MESH)
        copy.start()
        copies.append(copy)
        return copy

    tables_ref[me] = own_table_ref[...]
    shared = [send(own_table_ref, tables_ref.at[me], {'ep': peer}) for peer in (partner, across, diagonal)]
    for copy in shared:
        copy.wait_recv()
    for owner in range(tables_ref.shape[0]):
        table_ref[owner] = tables_ref[owner].T

    owners = (diagonal, across, partner, me) * HALVES
    fill_blocks = half // FILL_ROWS

    def fill(job, block):
        fill_gate_block(table_ref.at[owners[job]], job // 4 * half, first_code, terms_refs[job % GATE_SLOTS], block)

    def partial_sums(job, first, cols, dst_ref=None, extra_ref=None, resid=None, keep_ref=None, ahead=None):
        steps, begin = cols // PART_COLS, first // PART_COLS
        owner = owners[job]

        def body(block_ref, *refs):
            block = block_ref[...].reshape(experts * slot_dev, PART_COLS)
            sums = jnp.dot(terms_refs[job % GATE_SLOTS][...], block, preferred_element_type=jnp.float32)
            total = sums[:half] + (sums[half:2 * half] + sums[2 * half:])
            at = pl.ds(pl.multiple_of((pl.program_id(0) + begin) * PART_COLS, PART_COLS), PART_COLS)
            if extra_ref is not None:
                total = total + extra_ref[:, at]
            if resid is not None:
                total = refs[0][...].astype(jnp.float32) + total
            if keep_ref is not None:
                keep_ref[:, at] = total
            else:
                refs[-1][...] = total
            if ahead is not None:
                per_step = fill_blocks // steps
                for i in range(per_step):
                    fill(ahead, pl.program_id(0) * per_step + i)

        col_spec = pl.BlockSpec((half, PART_COLS), lambda n: (0, n + begin))
        in_specs = [pl.BlockSpec((experts, slot_dev, PART_COLS), lambda n: (0, owner, n + begin))]
        operands = [out_rows_ref]
        if resid is not None:
            in_specs.append(col_spec)
            operands.append(resid)
        if keep_ref is None:
            pltpu.emit_pipeline(body, grid=(steps,), in_specs=in_specs, out_specs=[col_spec])(*operands, dst_ref)
        else:
            pltpu.emit_pipeline(body, grid=(steps,), in_specs=in_specs)(*operands)

    def col_span(first, cols):
        return (slice(None), pl.ds(first, cols))

    def half_rows(part):
        return pl.ds(part * half, half)

    def pair_part(part, first, cols, ahead=None, after=None):
        source = pair_out_ref.at[part]
        partial_sums(4 * part, first, cols, source, ahead=ahead)
        if after is not None:
            after.wait_recv()
        span = col_span(first, cols)
        return send(source.at[span], pair_in_ref.at[span], {'ep': partner})

    def cross_part(part, first, cols, pair, ahead=None):
        pair.wait_recv()
        source = cross_out_ref.at[part]
        partial_sums(4 * part + 1, first, cols, source, extra_ref=pair_in_ref, ahead=ahead)
        for at in range(first, first + cols, SEND_COLS):
            span = col_span(at, SEND_COLS)
            crossed[part].append(send(source.at[span], cross_in_ref.at[part].at[span], {'ep': across}))

    def near_part(part, ahead=None):
        source = near_out_ref.at[part]
        partial_sums(4 * part + 2, 0, model_dim, source, ahead=ahead)
        return send(source, near_in_ref, {'ep': partner})

    def base_part(part, ahead=None):
        partial_sums(4 * part + 3, 0, model_dim, extra_ref=near_in_ref, resid=resid_ref.at[half_rows(part)], keep_ref=base_ref, ahead=ahead)

    def finish(part, index):
        if part > 0:
            moved[part - 1][index].wait_send()
        crossed[part][index].wait_recv()
        span = col_span(index * SEND_COLS, SEND_COLS)
        combined_ref[span] = (base_ref[span] + cross_in_ref[(part,) + span]).astype(jnp.bfloat16)
        target = arrived_ref.at[half_rows(part), pl.ds(index * SEND_COLS, SEND_COLS)]
        moved[part].append(send(combined_ref.at[span], target, {'pp': next_stage}))

    crossed = [[], []]
    moved = [[], []]
    chunks = model_dim // SEND_COLS
    one, rest = SEND_COLS, model_dim - 2 * SEND_COLS

    @pl.loop(0, fill_blocks)
    def _(block):
        fill(0, block)

    pair_a = pair_part(0, 0, one, ahead=1)
    cross_part(0, 0, one, pair_a)
    pair_b = pair_part(0, one, one)
    pair_c = pair_part(0, 2 * one, rest, ahead=2)
    cross_part(0, one, one, pair_b)
    cross_part(0, 2 * one, rest, pair_c, ahead=3)
    near = near_part(0, ahead=4)
    middle = model_dim // 2
    pair_d = pair_part(1, 0, middle, after=near)
    base_part(0, ahead=5)
    finish(0, 0)
    finish(0, 1)
    pair_e = pair_part(1, middle, middle, ahead=6)
    finish(0, 2)
    cross_part(1, 0, middle, pair_d, ahead=7)
    for index in range(3, chunks):
        finish(0, index)
    cross_part(1, middle, middle, pair_e)
    near = near_part(1)

    for copy in moved[0]:
        copy.wait_recv()
    load = pltpu.make_async_copy(arrived_ref.at[half_rows(0)], x_ref, load_sem)
    load.start()
    load.wait()
    normalise(x_ref, gain_ref, normed_ref)

    group = HEAD_GROUP * head_dim
    groups = k_ref.shape[1] // group

    def head_groups(first, count):
        def body(wq_block, wk_block, wv_block, k_block, v_block, context_block):
            scores = head_scores(q_held_ref, [k_held_ref], head_dim)
            queries = project_block(normed_ref, wq_block)
            keys = project_block(normed_ref, wk_block)
            head_context(scores, [v_held_ref], head_dim, context_block)
            values = project_block(normed_ref, wv_block)
            k_block[...] = keys
            v_block[...] = values
            q_held_ref[...] = queries
            k_held_ref[...] = keys
            v_held_ref[...] = values

        out_spec = pl.BlockSpec((half, group), lambda n: (0, n + first))
        late_spec = pl.BlockSpec((half, group), lambda n: (0, jnp.maximum(n + first - 1, 0)))
        pltpu.emit_pipeline(
            body, grid=(count,), in_specs=[weight_spec_at(model_dim, group, first)] * 3, out_specs=[out_spec, out_spec, late_spec],
        )(wq_ref, wk_ref, wv_ref, k_ref, v_ref, context_ref.at[half_rows(0)])

    def last_group(context_block):
        attend_heads(q_held_ref, [k_held_ref], [v_held_ref], head_dim, context_block)

    for ref in (q_held_ref, k_held_ref, v_held_ref):
        ref[...] = jnp.zeros_like(ref)
    third = groups // 3
    head_groups(0, third)
    near.wait_recv()
    base_part(1)
    finish(1, 0)
    finish(1, 1)
    head_groups(third, third)
    for index in range(2, chunks):
        finish(1, index)
    head_groups(2 * third, groups - 2 * third)
    pltpu.emit_pipeline(last_group, grid=(1,), out_specs=[pl.BlockSpec((half, group), lambda n: (0, groups - 1))])(
        context_ref.at[half_rows(0)])
    for copy in moved[1]:
        copy.wait_recv()
    already = {id(copy) for copy in moved[0]}
    for copy in copies:
        if id(copy) not in already:
            copy.wait_send()


def exchange(own_table, ep_size, own_out, own_resid, gain, w_query, w_key, w_value, head_dim):
    seq, model_dim = own_resid.shape
    hidden = w_query.shape[1]
    half = seq // HALVES
    slots = own_out.shape[0] * own_out.shape[1] // ep_size
    staged = jax.ShapeDtypeStruct((HALVES, half, model_dim), jnp.float32)
    out_shape = [
        jax.ShapeDtypeStruct((seq, model_dim), jnp.bfloat16),
        jax.ShapeDtypeStruct((half, hidden), jnp.bfloat16),
        jax.ShapeDtypeStruct((half, hidden), jnp.bfloat16),
        jax.ShapeDtypeStruct((seq, hidden), jnp.bfloat16),
        staged, staged, staged,
    ]
    chunks = model_dim // SEND_COLS
    n_copies = 3 + 5 + 2 + 2 * HALVES * chunks
    outs = pl.pallas_call(
        functools.partial(exchange_kernel, head_dim),
        out_shape=out_shape,
        in_specs=[VMEM_SPEC, ANY_SPEC, ANY_SPEC, VMEM_SPEC, ANY_SPEC, ANY_SPEC, ANY_SPEC],
        out_specs=[ANY_SPEC] * len(out_shape),
        scratch_shapes=[
            *[pltpu.VMEM((3 * half, slots), jnp.bfloat16)] * GATE_SLOTS,
            pltpu.VMEM((ep_size,) + own_table.shape, jnp.float32),
            pltpu.VMEM((ep_size,) + own_table.shape[::-1], jnp.float32),
            pltpu.VMEM((half, model_dim), jnp.float32),
            pltpu.VMEM((half, model_dim), jnp.float32),
            pltpu.VMEM((HALVES, half, model_dim), jnp.float32),
            pltpu.VMEM((half, model_dim), jnp.float32),
            pltpu.VMEM((half, model_dim), jnp.bfloat16),
            pltpu.VMEM((half, model_dim), jnp.bfloat16),
            pltpu.VMEM((half, model_dim), jnp.bfloat16),
            *[pltpu.VMEM((half, HEAD_GROUP * head_dim), jnp.bfloat16)] * 3,
            pltpu.SemaphoreType.DMA,
            pltpu.SemaphoreType.DMA((n_copies,)),
            pltpu.SemaphoreType.DMA((n_copies,)),
        ],
        compiler_params=pltpu.CompilerParams(vmem_limit_bytes=VMEM_LIMIT, collective_id=0, has_side_effects=True),
        name="exchange",
    )(own_table, own_out, own_resid, gain, w_query, w_key, w_value)
    return outs[:4]


def second_half_kernel(head_dim, gain_ref, x_ref, wq_ref, wk_ref, wv_ref, k_ref, v_ref, held_ref, context_ref,
                       normed_ref, q_held_ref, k_held_ref, v_held_ref):
    del held_ref
    half, model_dim = x_ref.shape
    normalise(x_ref, gain_ref, normed_ref)
    group = LAST_GROUP * head_dim
    groups = k_ref.shape[1] // group
    for ref in (q_held_ref, k_held_ref, v_held_ref):
        ref[...] = jnp.zeros_like(ref)

    def attend_before(k_block, v_block, context_block):
        attend_heads(q_held_ref, [k_block, k_held_ref], [v_block, v_held_ref], head_dim, context_block)

    def body(wq_block, wk_block, wv_block, k_block, v_block, context_block):
        scores = head_scores(q_held_ref, [k_block, k_held_ref], head_dim)
        queries = project_block(normed_ref, wq_block)
        keys = project_block(normed_ref, wk_block)
        head_context(scores, [v_block, v_held_ref], head_dim, context_block)
        values = project_block(normed_ref, wv_block)
        q_held_ref[...] = queries
        k_held_ref[...] = keys
        v_held_ref[...] = values

    late_spec = pl.BlockSpec((half, group), lambda n: (0, jnp.maximum(n - 1, 0)))
    last_spec = pl.BlockSpec((half, group), lambda n: (0, groups - 1))
    target = context_ref.at[pl.ds(half, half)]
    pltpu.emit_pipeline(
        body, grid=(groups,), in_specs=[weight_spec_at(model_dim, group, 0)] * 3 + [late_spec] * 2, out_specs=[late_spec],
    )(wq_ref, wk_ref, wv_ref, k_ref, v_ref, target)
    pltpu.emit_pipeline(attend_before, grid=(1,), in_specs=[last_spec] * 2, out_specs=[last_spec])(k_ref, v_ref, target)


def second_half(arrived, gain, w_query, w_key, w_value, keys, values, context, head_dim):
    seq, model_dim = arrived.shape
    hidden = w_query.shape[1]
    half = seq // HALVES
    return pl.pallas_call(
        functools.partial(second_half_kernel, head_dim),
        out_shape=jax.ShapeDtypeStruct(context.shape, context.dtype),
        grid=(1,),
        in_specs=[pl.BlockSpec(gain.shape, lambda n: (0, 0)), pl.BlockSpec((half, model_dim), lambda n: (1, 0))] + [ANY_SPEC] * 6,
        out_specs=ANY_SPEC,
        input_output_aliases={7: 0},
        scratch_shapes=[pltpu.VMEM((half, model_dim), jnp.bfloat16)] + [pltpu.VMEM((half, LAST_GROUP * head_dim), jnp.bfloat16)] * 3,
        compiler_params=pltpu.CompilerParams(vmem_limit_bytes=VMEM_LIMIT, dimension_semantics=("arbitrary",)),
        cost_estimate=pl.CostEstimate(flops=6 * half * model_dim * hidden, bytes_accessed=6 * model_dim * hidden, transcendentals=0),
        name="second_half",
    )(gain, arrived, w_query, w_key, w_value, keys, values, context)


def solution(mesh):
    ep_size = mesh.shape['ep']
    token_spec = P(('data', 'pp'), None, 'ep', None, None)
    weight_spec = P('pp', None, None)

    def local_step(expert_out, expert_ids, slot_ids, gates, resid, norm_scale, w_query, w_key, w_value, w_out):
        own_out = expert_out[0, 0]
        own_resid = resid[0, 0, 0]
        model_dim = own_out.shape[2]
        slot_dev = own_out.shape[1] // ep_size
        me = lax.axis_index('ep')
        ids, slots, own_gates = expert_ids[0, 0, 0], slot_ids[0, 0, 0], gates[0, 0, 0]
        code = jnp.where(slots >= 0, ids * slot_dev + (slots - me * slot_dev), -1).astype(jnp.float32)
        own_table = jnp.concatenate([code.T, own_gates.T], axis=0)
        gain = norm_scale.reshape(1, model_dim)
        head_count, head_dim = w_out.shape[1], w_out.shape[2]
        weights = (w_query[0], w_key[0], w_value[0])
        arrived, keys, values, context = exchange(own_table, ep_size, own_out, own_resid, gain, *weights, head_dim)
        context = second_half(arrived, gain, *weights, keys, values, context, head_dim)
        flat_out = w_out[0].reshape(head_count * head_dim, model_dim)
        proj = jnp.dot(context, flat_out, preferred_element_type=jnp.float32).astype(jnp.bfloat16)
        result = (arrived.astype(jnp.float32) + proj.astype(jnp.float32)).astype(jnp.bfloat16)
        return result[None, None, None]

    return jax.shard_map(local_step, mesh=mesh, in_specs=(token_spec, token_spec, token_spec, token_spec, token_spec, P('pp', None), weight_spec, weight_spec, weight_spec, P('pp', None, None, None)), out_specs=token_spec, check_vma=False)
```
